32 devices in a mesh: gx: 4 (over y, x), gy: 2 (over core), gz: 4 (over z).
Axes of the slice: x: 2, y: 2, z: 4, core: 2. Of those that a mesh axis runs over, the one named last changes fastest.
Arguments:
- pair: bfloat16 [128, 1024, 1024], P('gz', 'gy', 'gx'), may hold values from -6 to 6
- pair_mask: int32 [1024, 1024], P('gy', 'gx'), may hold values 0 or 1
- in_gain: float32 [128], replicated, may hold values from 0.5 to 2
- w_left: bfloat16 [128, 128], P(None, 'gz'), may hold values from -0.5 to 0.5
- w_left_gate: bfloat16 [128, 128], P(None, 'gz'), may hold values from -0.5 to 0.5
- w_right: bfloat16 [128, 128], P(None, 'gz'), may hold values from -0.5 to 0.5
- w_right_gate: bfloat16 [128, 128], P(None, 'gz'), may hold values from -0.5 to 0.5
- w_out_gate: bfloat16 [128, 128], P(None, 'gz'), may hold values from -0.5 to 0.5
- out_gain: float32 [128], P('gz'), may hold values from 0.5 to 2
- w_out: bfloat16 [128, 128], P(None, 'gz'), may hold values from -0.5 to 0.5
Outputs:
- update: bfloat16 [128, 1024, 1024], P('gz', 'gy', 'gx')
The draws below stay inside these ranges and needn't reach their ends.
All inputs are finite; a program needn't handle non-finite values. No bound on the sum of `pair_mask` on one device may be relied on, other than what follows from the above.
Results may differ from the reference program's by a relative error of at most 0.0078.
Values may be sent and summed in bfloat16 or wider, within the bound.
A program may use at most 192 MiB of HBM per device.

```python
import math
import jax
import jax.numpy as jnp
from jax import lax

CZ = 128
CH = 128
N = 1024


def set_ends(values, own_key, smallest, high):
    longest = values.shape.index(max(values.shape))
    spots = []
    for shift in (0, 1):
        where = [jax.random.randint(jax.random.fold_in(own_key, axis), (), 0, length) for axis, length in enumerate(values.shape)]
        where[longest] = (where[longest] + shift) % values.shape[longest]
        spots.append(tuple(where))
    return values.at[spots[0]].set(smallest).at[spots[1]].set(high)


def block_levels(own_key, shape, shards, least, top_value):
    level, own = 1.0, jax.random.fold_in(own_key, 6)
    for dim, shards_of in shards:
        steps = jnp.exp(jax.random.uniform(jax.random.fold_in(own, dim), (shards_of,), jnp.float32, least / len(shards), top_value / len(shards)))
        level = level * jnp.repeat(steps, shape[dim] // shards_of).reshape([-1 if axis == dim else 1 for axis in range(len(shape))])
    return level


def normal_values(key, dims, deviation, bound, cuts=(), held_as=jnp.bfloat16):
    entries = jax.random.normal(key, dims, jnp.float32) * deviation
    if len(cuts) > 0:
        entries = block_levels(key, dims, cuts, -0.22, 0.18) * entries
    return jnp.clip(entries, min=-bound, max=bound).astype(held_as)


def setup_inputs(seed: int = 0) -> dict:
    arg_keys = jax.random.split(jax.random.key(seed), 11)
    pair = normal_values(arg_keys[0], (CZ, N, N), 1.0, 6.0, ((0, 4), (1, 2), (2, 4)))
    pair_mask = set_ends((jax.random.randint(arg_keys[1], (N, N), 0, 8) < 7).astype(jnp.int32), jax.random.fold_in(arg_keys[1], 1), 0, 1)
    in_gain = jnp.clip(jnp.exp(jax.random.uniform(arg_keys[2], (CZ,), jnp.float32, math.log(0.5), math.log(2.0))), 0.5, 2.0)
    w_left = normal_values(arg_keys[3], (CZ, CH), CZ ** -0.5, 0.5, ((1, 4),))
    w_left_gate = normal_values(arg_keys[4], (CZ, CH), CZ ** -0.5, 0.5, ((1, 4),))
    w_right = normal_values(arg_keys[5], (CZ, CH), CZ ** -0.5, 0.5, ((1, 4),))
    w_right_gate = normal_values(arg_keys[6], (CZ, CH), CZ ** -0.5, 0.5, ((1, 4),))
    w_out_gate = normal_values(arg_keys[7], (CZ, CZ), CZ ** -0.5, 0.5, ((1, 4),))
    out_gain = jnp.clip(jnp.exp(math.log(2.0) - 1.3862944 * jax.random.uniform(arg_keys[8], (CH,), jnp.float32) ** block_levels(arg_keys[8], (CH,), ((0, 4),), -0.2, 0.2)), 0.5, 2.0)
    w_out = normal_values(arg_keys[9], (CH, CZ), CH ** -0.5, 0.5, ((1, 4),))
    return {"pair": pair, "pair_mask": pair_mask, "in_gain": in_gain, "w_left": w_left, "w_left_gate": w_left_gate, "w_right": w_right, "w_right_gate": w_right_gate, "w_out_gate": w_out_gate, "out_gain": out_gain, "w_out": w_out}


epsilon = 1e-05

def layer_norm(values, gain):
    average = lax.optimization_barrier(jnp.mean(values, axis=0))
    centered = values - average
    spread = lax.optimization_barrier(jnp.mean(jnp.square(centered), axis=0))
    return centered * lax.rsqrt(spread + epsilon) * gain[:, None, None]

def reference(pair, pair_mask, in_gain, w_left, w_left_gate, w_right, w_right_gate, w_out_gate, out_gain, w_out):
    normed = layer_norm(pair.astype(jnp.float32), in_gain).astype(jnp.bfloat16)
    normed_f = normed.astype(jnp.float32)
    mask_float = pair_mask.astype(jnp.float32)[None]

    def project(weight):
        return jnp.einsum('cik,ch->hik', normed_f, weight.astype(jnp.float32))
    left_rows = (mask_float * jax.nn.sigmoid(project(w_left_gate)) * project(w_left)).astype(jnp.bfloat16)
    right_rows = (mask_float * jax.nn.sigmoid(project(w_right_gate)) * project(w_right)).astype(jnp.bfloat16)

    def channel_product(operands):
        return jnp.dot(operands[0], operands[1].T, preferred_element_type=jnp.float32)
    mixed_sum = lax.map(channel_product, (left_rows, right_rows))
    normed_mix = layer_norm(mixed_sum, out_gain).astype(jnp.bfloat16)
    out_gate = jax.nn.sigmoid(jnp.einsum('cij,cd->dij', normed_f, w_out_gate.astype(jnp.float32)))
    projected = jnp.einsum('hij,hd->dij', normed_mix.astype(jnp.float32), w_out.astype(jnp.float32))
    return (out_gate * projected).astype(jnp.bfloat16)
```

```python
import functools

import jax
import jax.numpy as jnp
from jax import lax
from jax.experimental import pallas as pl
from jax.experimental.pallas import tpu as pltpu
from jax.sharding import PartitionSpec as P

epsilon = 1e-05
MESH = pl.DeviceIdType.MESH
LANES = 128
GROUP = 16
PITCH = GROUP + 1
VMEM_LIMIT = 67043328


def normalize(values, gain):
    average = jnp.mean(values, axis=0, keepdims=True)
    centered = values - average
    spread = jnp.mean(jnp.square(centered), axis=0, keepdims=True)
    return (centered * lax.rsqrt(spread + epsilon) * gain).astype(jnp.bfloat16)


class Place:
    def __init__(self, nx, ny, nz):
        self.nx, self.ny, self.nz = nx, ny, nz
        self.gx, self.gy, self.gz = (lax.axis_index(a) for a in ("gx", "gy", "gz"))
        self.group = self.gx * ny + self.gy
        self.groups = nx * ny
        self.side = self.gz // (nz // 2)
        self.mid = nz // 2 - 1 + self.side
        self.far = self.side * (nz - 1)
        self.is_mid = self.gz == self.mid
        self.is_far = jnp.logical_and(self.gz == self.far, jnp.logical_not(self.is_mid))

    def member(self, offset):
        q = lax.rem(self.group + offset, self.groups)
        return q, q // self.ny, lax.rem(q, self.ny)


def remote(src, dst, send, recv, **device):
    return pltpu.make_async_remote_copy(
        src_ref=src, dst_ref=dst, send_sem=send, recv_sem=recv, device_id=device, device_id_type=MESH
    )


def turn_out(slab, stage_of, count):
    def body(i, carry):
        for u in range(8):
            h = i * 8 + u
            for part in range(slab.shape[0]):
                rows = slab.at[part][pl.ds(h * PITCH, GROUP), :]
                stage_of(h, part, rows.astype(jnp.bfloat16))
        return carry

    lax.fori_loop(0, count // 8, body, 0)


def put_strided(slab, row, values):
    for part in range(slab.shape[0]):
        slab.at[part][pl.ds(row, values.shape[0], stride=PITCH), :] = values[
            :, part * LANES : (part + 1) * LANES
        ]


def project_kernel(
    dims,
    pair_ref,
    mask_ref,
    gain_ref,
    weight_ref,
    right_ref,
    left_ref,
    gate_ref,
    raw,
    right_stage,
    left_stage,
    gate_stage,
    right_slab,
    left_slab,
    raw_send,
    raw_recv,
    own_sem,
    right_send,
    left_send,
    right_recv,
    left_recv,
    gate_sem,
):
    nx, ny, nz, near, away = dims
    at = Place(nx, ny, nz)
    rows, c, k = pair_ref.shape
    h = weight_ref.shape[0] // 5
    size = right_stage.shape[2]
    chunks = rows // size
    half = chunks // 2
    per = near + away
    ahead = min(4, chunks)

    def row_of(t, side):
        return pl.multiple_of(lax.rem(t + side * half, chunks) * size, size)

    def raw_copy(t, side):
        r = row_of(t, side)
        return remote(
            pair_ref.at[pl.ds(r, size)],
            raw.at[pl.ds(r, size), pl.ds(pl.multiple_of(at.gz * c, c), c)],
            raw_send.at[t, side],
            raw_recv.at[lax.rem(t + side * half, chunks), at.gz],
            gz=nz // 2 - 1 + side,
        )

    def raw_wait(t, z):
        r = row_of(t, at.side)
        remote(
            pair_ref.at[pl.ds(r, size)],
            raw.at[pl.ds(r, size), pl.ds(pl.multiple_of(z * c, c), c)],
            raw_send.at[t, 0],
            raw_recv.at[lax.rem(t + at.side * half, chunks), z],
            gz=z,
        ).wait_recv()

    def sends(stage, out_ref, block, send, recv, slot, r):
        first = pl.multiple_of(at.gy * block + r, size)
        where = (pl.ds(first, size), pl.ds(pl.multiple_of(at.gx * k, k), k))
        found = []
        for o in range(at.groups):
            q, qx, qy = at.member(o)
            src = stage.at[slot, pl.ds(q * per, near)]
            dst = out_ref.at[(pl.ds(0, near),) + where]
            if o == 0:
                found.append((pltpu.make_async_copy(src, dst, send.at[slot, 0]), True))
            else:
                found.append((remote(src, dst, send.at[slot, o], recv.at[at.group], gx=qx, gy=qy), False))
            if away:
                found.append(
                    (
                        remote(
                            stage.at[slot, pl.ds(q * per + near, away)],
                            out_ref.at[(pl.ds(0, away),) + where],
                            send.at[slot, at.groups + o],
                            recv.at[at.group],
                            gx=qx,
                            gy=qy,
                            gz=at.far,
                        ),
                        False,
                    )
                )
        return found

    def right_sends(t):
        return sends(
            right_stage, right_ref, rows, right_send, right_recv, lax.rem(t, 2), row_of(t, at.side)
        )

    def left_sends(t):
        return sends(left_stage, left_ref, rows // 2, left_send, left_recv, lax.rem(t, 2), t * size)

    def gate_copy(t):
        slot = lax.rem(t, 2)
        return pltpu.make_async_copy(
            gate_stage.at[slot], gate_ref.at[pl.ds(t * size, size)], gate_sem.at[slot]
        )

    def start(copies):
        for copy, _ in copies:
            copy.start()

    def drain(copies):
        for copy, is_local in copies:
            if is_local:
                copy.wait()
            else:
                copy.wait_send()

    def compute(t, with_left):
        slot = lax.rem(t, 2)
        r0 = row_of(t, at.side)
        gain = gain_ref[...]
        for g in range(size // GROUP):

            def body(r, carry):
                row = r0 + g * GROUP + r
                normed = normalize(raw[row].astype(jnp.float32), gain)
                mask = mask_ref[pl.ds(row, 1), :]

                def part(index):
                    return jnp.dot(
                        weight_ref[index * h : (index + 1) * h, :],
                        normed,
                        preferred_element_type=jnp.float32,
                    )

                put_strided(right_slab, r, mask * jax.nn.sigmoid(part(3)) * part(2))
                if with_left:
                    put_strided(left_slab, r, mask * jax.nn.sigmoid(part(1)) * part(0))
                    gate_stage[slot, g * GROUP + r] = jax.nn.sigmoid(part(4)).astype(jnp.bfloat16)
                return carry

            lax.fori_loop(0, GROUP, body, 0)

            def stage_into(stage):
                def put(head, part, values):
                    stage[
                        slot,
                        head,
                        g * GROUP : (g + 1) * GROUP,
                        part * LANES : (part + 1) * LANES,
                    ] = values

                return put

            turn_out(right_slab, stage_into(right_stage), h)
            if with_left:
                turn_out(left_slab, stage_into(left_stage), h)

    def arrive(t):
        for o in range(1, nz):
            raw_wait(t, lax.rem(at.gz + o, nz))

    @pl.when(jnp.logical_not(at.is_mid))
    def _():
        def begin(t, carry):
            raw_copy(t, 0).start()
            raw_copy(t, 1).start()
            return carry

        def end(t, carry):
            raw_copy(t, 0).wait_send()
            raw_copy(t, 1).wait_send()
            return carry

        lax.fori_loop(0, chunks, begin, 0)
        lax.fori_loop(0, chunks, end, 0)

    @pl.when(at.is_mid)
    def _():
        other = 1 - at.side
        own = pltpu.make_async_copy(
            pair_ref, raw.at[:, pl.ds(pl.multiple_of(at.gz * c, c), c)], own_sem
        )
        own.start()
        for t in range(ahead):
            raw_copy(t, other).start()
        own.wait()

        def step(t, with_left):
            @pl.when(t + ahead < chunks)
            def _():
                raw_copy(t + ahead, other).start()

            arrive(t)

            @pl.when(t >= 2)
            def _():
                drain(right_sends(t - 2))
                if with_left:
                    drain(left_sends(t - 2))
                    gate_copy(t - 2).wait()

            compute(t, with_left)
            start(right_sends(t))
            if with_left:
                start(left_sends(t))
                gate_copy(t).start()

        def first(t, carry):
            step(t, True)
            return carry

        def second(t, carry):
            step(t, False)
            return carry

        lax.fori_loop(0, half, first, 0)
        lax.fori_loop(half, chunks, second, 0)
        for t in range(max(half - 2, 0), half):
            drain(left_sends(t))
            gate_copy(t).wait()
        for t in range(max(chunks - 2, 0), chunks):
            drain(right_sends(t))

        def end(t, carry):
            raw_copy(t, other).wait_send()
            return carry

        lax.fori_loop(0, chunks, end, 0)

    def collect(heads, first_offset):
        for o in range(first_offset, at.groups):
            q, qx, qy = at.member(o)
            for out_ref, block, recv in (
                (right_ref, rows, right_recv),
                (left_ref, rows // 2, left_recv),
            ):
                whole = out_ref.at[
                    pl.ds(0, heads),
                    pl.ds(pl.multiple_of(qy * block, block), block),
                    pl.ds(pl.multiple_of(qx * k, k), k),
                ]
                remote(whole, whole, own_sem, recv.at[q], gz=at.mid).wait_recv()

    @pl.when(at.is_mid)
    def _():
        collect(near, 1)

    if away:

        @pl.when(at.is_far)
        def _():
            collect(away, 0)


def mix_kernel(
    dims,
    right_ref,
    left_ref,
    gate_ref,
    gain_ref,
    weight_ref,
    out_ref,
    right,
    left,
    stage,
    mix,
    gate,
    out_stage,
    in_slab,
    out_slab,
    right_sem,
    left_sem,
    gate_sem,
    mix_send,
    mix_recv,
    out_send,
    out_recv,
):
    nx, ny, nz, near, away = dims
    at = Place(nx, ny, nz)
    c, rows, k = out_ref.shape
    h = weight_ref.shape[0]
    own_rows = rows // 2
    steps = own_rows // GROUP
    per = near + away
    deep = max(near, away)

    def left_copies(t, heads):
        slot = lax.rem(t, 2)
        return [
            pltpu.make_async_copy(
                left_ref.at[pl.ds(0, heads), pl.ds(pl.multiple_of(y * own_rows + t * GROUP, GROUP), GROUP)],
                left.at[slot, pl.ds(0, heads), pl.ds(y * GROUP, GROUP)],
                left_sem.at[slot, y],
            )
            for y in range(ny)
        ]

    def right_copy(head):
        return pltpu.make_async_copy(right_ref.at[head], right.at[head], right_sem.at[head])

    def gate_copy(t):
        slot = lax.rem(t, 2)
        return pltpu.make_async_copy(
            gate_ref.at[pl.ds(t * GROUP, GROUP)], gate.at[slot], gate_sem.at[slot]
        )

    def mix_sends(t, heads, shift, first_offset):
        slot = lax.rem(t, 2)
        found = []
        for o in range(first_offset, at.groups):
            q, qx, qy = at.member(o)
            found.append(
                remote(
                    stage.at[
                        slot,
                        pl.ds(0, heads),
                        pl.ds(pl.multiple_of(qy * GROUP, GROUP), GROUP),
                        pl.ds(pl.multiple_of(qx * k, k), k),
                    ],
                    mix.at[
                        pl.ds(at.group * per + shift, heads),
                        pl.ds(pl.multiple_of(t * GROUP, GROUP), GROUP),
                    ],
                    mix_send.at[slot, o],
                    mix_recv.at[t],
                    gx=qx,
                    gy=qy,
                    gz=at.mid,
                )
            )
        return found

    def multiply(t, heads, shift, first_offset):
        slot = lax.rem(t, 2)

        @pl.when(t + 1 < steps)
        def _():
            for copy in left_copies(t + 1, heads):
                copy.start()

        for copy in left_copies(t, heads):
            copy.wait()

        @pl.when(t >= 2)
        def _():
            for copy in mix_sends(t - 2, heads, shift, first_offset):
                copy.wait_send()

        def body(head, carry):
            @pl.when(t == 0)
            def _():
                right_copy(head).wait()

            product = lax.dot_general(
                left[slot, head],
                right[head],
                (((1,), (1,)), ((), ())),
                preferred_element_type=jnp.float32,
            )
            stage[slot, head] = product.astype(jnp.bfloat16)
            return carry

        lax.fori_loop(0, heads, body, 0)
        for copy in mix_sends(t, heads, shift, first_offset):
            copy.start()

    def begin(heads):
        for copy in left_copies(0, heads):
            copy.start()
        for head in range(heads):
            right_copy(head).start()

    def end(heads, shift, first_offset):
        for t in range(max(steps - 2, 0), steps):
            for copy in mix_sends(t, heads, shift, first_offset):
                copy.wait_send()

    def out_copies(t):
        slot = lax.rem(t, 2)
        where = pl.ds(pl.multiple_of(at.side * own_rows + t * GROUP, GROUP), GROUP)
        found = [
            (
                pltpu.make_async_copy(
                    out_stage.at[slot, pl.ds(pl.multiple_of(at.gz * c, c), c)],
                    out_ref.at[:, where],
                    out_send.at[slot, 0],
                ),
                True,
            )
        ]
        for o in range(1, nz):
            z = lax.rem(at.gz + o, nz)
            found.append(
                (
                    remote(
                        out_stage.at[slot, pl.ds(pl.multiple_of(z * c, c), c)],
                        out_ref.at[:, where],
                        out_send.at[slot, o],
                        out_recv.at[at.side],
                        gz=z,
                    ),
                    False,
                )
            )
        return found

    def drain_out(t):
        for copy, is_local in out_copies(t):
            if is_local:
                copy.wait()
            else:
                copy.wait_send()

    def finish(t):
        slot = lax.rem(t, 2)
        here = pl.ds(pl.multiple_of(t * GROUP, GROUP), GROUP)
        if h > near:
            rest = mix.at[pl.ds(0, h - near), here]
            remote(rest, rest, out_send.at[0, 0], mix_recv.at[t], gz=at.mid).wait_recv()

        gain = gain_ref[...]

        def turn_in(i, carry):
            for u in range(8):
                head = i * 8 + u
                for part in range(in_slab.shape[0]):
                    in_slab.at[part][pl.ds(head * PITCH, GROUP), :] = mix[
                        head, here, part * LANES : (part + 1) * LANES
                    ].astype(jnp.float32)
            return carry

        lax.fori_loop(0, h // 8, turn_in, 0)

        @pl.when(t + 1 < steps)
        def _():
            gate_copy(t + 1).start()

        gate_copy(t).wait()

        def body(r, carry):
            values = jnp.concatenate(
                [
                    in_slab.at[part][pl.ds(r, h, stride=PITCH), :]
                    for part in range(in_slab.shape[0])
                ],
                axis=1,
            )
            normed = normalize(values, gain)
            projected = jnp.dot(weight_ref[...], normed, preferred_element_type=jnp.float32)
            put_strided(out_slab, r, gate[slot, r].astype(jnp.float32) * projected)
            return carry

        lax.fori_loop(0, GROUP, body, 0)

        @pl.when(t >= 2)
        def _():
            drain_out(t - 2)

        def put(head, part, values):
            out_stage[slot, head, :, part * LANES : (part + 1) * LANES] = values

        turn_out(out_slab, put, h)
        for copy, _ in out_copies(t):
            copy.start()

    @pl.when(at.is_mid)
    def _():
        begin(near)
        gate_copy(0).start()

        def keep_own(t):
            slot = lax.rem(t, 2)
            mix[
                pl.ds(at.group * per, near), pl.ds(pl.multiple_of(t * GROUP, GROUP), GROUP)
            ] = stage[
                slot,
                0:near,
                pl.ds(pl.multiple_of(at.gy * GROUP, GROUP), GROUP),
                pl.ds(pl.multiple_of(at.gx * k, k), k),
            ]

        def step(t, carry):
            multiply(t, near, 0, 1)
            keep_own(t)

            @pl.when(t >= 1)
            def _():
                finish(t - 1)

            return carry

        lax.fori_loop(0, steps, step, 0)
        finish(jnp.int32(steps - 1))
        end(near, 0, 1)
        for t in range(max(steps - 2, 0), steps):
            drain_out(t)

    if away:

        @pl.when(at.is_far)
        def _():
            begin(away)

            def step(t, carry):
                multiply(t, away, near, 0)
                return carry

            lax.fori_loop(0, steps, step, 0)
            end(away, near, 0)

    for side in range(2):
        source = nz // 2 - 1 + side

        @pl.when(at.gz != source)
        def _():
            where = out_ref.at[:, pl.ds(side * own_rows, own_rows)]
            remote(where, where, out_send.at[0, 0], out_recv.at[side], gz=source).wait_recv()


def local(
    pair,
    pair_mask,
    in_gain,
    w_left,
    w_left_gate,
    w_right,
    w_right_gate,
    w_out_gate,
    out_gain,
    w_out,
):
    nx, ny, nz = (lax.axis_size(a) for a in ("gx", "gy", "gz"))
    c, rows, k = pair.shape
    c_all = c * nz
    h = w_left.shape[1] * nz
    groups = nx * ny
    per = h // groups
    away = 0 if nz < 4 else max(1, per * 5 // 16)
    near = per - away
    deep = max(near, away)
    dims = (nx, ny, nz, near, away)
    size = min(32, rows // 2)
    chunks = rows // size
    steps = rows // 2 // GROUP
    parts = k // LANES

    stacked = jnp.stack([w_left, w_left_gate, w_right, w_right_gate, w_out_gate, w_out])
    weights = jnp.swapaxes(lax.all_gather(stacked, "gz", axis=2, tiled=True), 1, 2)
    gain_mix = lax.all_gather(out_gain, "gz", axis=0, tiled=True)
    anywhere = pl.BlockSpec(memory_space=pl.ANY)
    vmem = pl.BlockSpec(memory_space=pltpu.VMEM)
    bf16 = lambda *shape: jax.ShapeDtypeStruct(shape, jnp.bfloat16)
    sem = pltpu.SemaphoreType.DMA
    slab = pltpu.VMEM((parts, h * PITCH, LANES), jnp.float32)
    params = pltpu.CompilerParams(has_side_effects=True, vmem_limit_bytes=VMEM_LIMIT)

    right, left, gate = pl.pallas_call(
        functools.partial(project_kernel, dims),
        out_shape=(
            bf16(deep, ny * rows, nx * k),
            bf16(deep, ny * rows // 2, nx * k),
            bf16(rows // 2, h, k),
        ),
        in_specs=[anywhere, vmem, vmem, vmem],
        out_specs=(anywhere, anywhere, anywhere),
        scratch_shapes=[
            pltpu.VMEM((rows, c_all, k), jnp.bfloat16),
            pltpu.VMEM((2, h, size, k), jnp.bfloat16),
            pltpu.VMEM((2, h, size, k), jnp.bfloat16),
            pltpu.VMEM((2, size, h, k), jnp.bfloat16),
            slab,
            slab,
            sem((chunks, 2)),
            sem((chunks, nz)),
            sem,
            sem((2, 2 * groups)),
            sem((2, 2 * groups)),
            sem((groups,)),
            sem((groups,)),
            sem((2,)),
        ],
        compiler_params=params,
    )(
        jnp.swapaxes(pair, 0, 1),
        pair_mask.astype(jnp.float32),
        in_gain[:, None],
        weights[:5].reshape(5 * h, c_all),
    )

    return pl.pallas_call(
        functools.partial(mix_kernel, dims),
        out_shape=bf16(c, rows, k),
        in_specs=[anywhere, anywhere, anywhere, vmem, vmem],
        out_specs=anywhere,
        scratch_shapes=[
            pltpu.VMEM((deep, ny * rows, nx * k), jnp.bfloat16),
            pltpu.VMEM((2, deep, ny * GROUP, nx * k), jnp.bfloat16),
            pltpu.VMEM((2, deep, ny * GROUP, ny * rows), jnp.bfloat16),
            pltpu.VMEM((h, rows // 2, k), jnp.bfloat16),
            pltpu.VMEM((2, GROUP, h, k), jnp.bfloat16),
            pltpu.VMEM((2, h, GROUP, k), jnp.bfloat16),
            slab,
            slab,
            sem((deep,)),
            sem((2, ny)),
            sem((2,)),
            sem((2, groups)),
            sem((steps,)),
            sem((2, nz)),
            sem((2,)),
        ],
        compiler_params=params,
    )(right, left, gate, gain_mix[:, None], weights[5])


def solution(mesh):
    placed = (
        P("gz", "gy", "gx"),
        P("gy", "gx"),
        P(),
        P(None, "gz"),
        P(None, "gz"),
        P(None, "gz"),
        P(None, "gz"),
        P(None, "gz"),
        P("gz"),
        P(None, "gz"),
    )
    return jax.shard_map(
        local, mesh=mesh, in_specs=placed, out_specs=P("gz", "gy", "gx"), check_vma=False
    )
```

```python
import functools

import jax
import jax.numpy as jnp
from jax import lax
from jax.experimental import pallas as pl
from jax.experimental.pallas import tpu as pltpu
from jax.sharding import PartitionSpec as P

epsilon = 1e-05
MESH = pl.DeviceIdType.MESH
LANES = 128
GROUP = 16
PITCH = GROUP + 1
SLOTS = 4
LAG = 3
VMEM_LIMIT = 67043328


def normalize(values, gain):
    average = jnp.mean(values, axis=0, keepdims=True)
    centered = values - average
    spread = jnp.mean(jnp.square(centered), axis=0, keepdims=True)
    return (centered * lax.rsqrt(spread + epsilon) * gain).astype(jnp.bfloat16)


class Place:
    def __init__(self, nx, ny, nz):
        self.nx, self.ny, self.nz = nx, ny, nz
        self.gx, self.gy, self.gz = (lax.axis_index(a) for a in ("gx", "gy", "gz"))
        self.group = self.gx * ny + self.gy
        self.groups = nx * ny
        self.side = self.gz // (nz // 2)
        self.mid = nz // 2 - 1 + self.side
        self.far = self.side * (nz - 1)
        self.is_mid = self.gz == self.mid
        self.is_far = jnp.logical_and(self.gz == self.far, jnp.logical_not(self.is_mid))

    def member(self, offset):
        q = lax.rem(self.group + offset, self.groups)
        return q, q // self.ny, lax.rem(q, self.ny)


def remote(src, dst, send, recv, **device):
    return pltpu.make_async_remote_copy(
        src_ref=src, dst_ref=dst, send_sem=send, recv_sem=recv, device_id=device, device_id_type=MESH
    )


def same_place(n):
    return lax.broadcasted_iota(jnp.int32, (n, n), 0) == lax.broadcasted_iota(jnp.int32, (n, n), 1)


def column(row):
    return jnp.sum(jnp.where(same_place(row.shape[1]), row, 0.0), axis=1, keepdims=True)


def turn_in(slab, source, count):
    def body(i, carry):
        for u in range(8):
            channel = i * 8 + u
            for part in range(slab.shape[0]):
                slab.at[part][pl.ds(channel * PITCH, GROUP), :] = source(channel, part).astype(
                    jnp.float32
                )
        return carry

    lax.fori_loop(0, count // 8, body, 0)


def get_strided(slab, row, count):
    return jnp.concatenate(
        [slab.at[part][pl.ds(row, count, stride=PITCH), :] for part in range(slab.shape[0])], axis=1
    )


def turn_out(slab, stage_of, count):
    def body(i, carry):
        for u in range(8):
            h = i * 8 + u
            for part in range(slab.shape[0]):
                rows = slab.at[part][pl.ds(h * PITCH, GROUP), :]
                stage_of(h, part, rows.astype(jnp.bfloat16))
        return carry

    lax.fori_loop(0, count // 8, body, 0)


def put_strided(slab, row, values):
    for part in range(slab.shape[0]):
        slab.at[part][pl.ds(row, values.shape[0], stride=PITCH), :] = values[
            :, part * LANES : (part + 1) * LANES
        ]


def project_kernel(
    dims,
    pair_ref,
    mask_ref,
    gain_ref,
    w0_ref,
    w1_ref,
    w2_ref,
    w3_ref,
    w4_ref,
    right_ref,
    left_ref,
    gate_ref,
    raw,
    weight_ref,
    right_stage,
    left_stage,
    gate_stage,
    raw_slab,
    right_slab,
    left_slab,
    raw_send,
    raw_recv,
    weight_send,
    weight_recv,
    own_sem,
    right_send,
    left_send,
    right_recv,
    left_recv,
    gate_sem,
):
    nx, ny, nz, near, away = dims
    at = Place(nx, ny, nz)
    c, rows, k = pair_ref.shape
    given = (w0_ref, w1_ref, w2_ref, w3_ref, w4_ref)
    h_z, c_all = w0_ref.shape
    h = h_z * nz
    size = right_stage.shape[2]
    chunks = rows // size
    half = chunks // 2
    per = near + away
    ahead = min(6, chunks)

    def row_of(t, side):
        return pl.multiple_of(lax.rem(t + side * half, chunks) * size, size)

    def raw_copy(t, side):
        r = row_of(t, side)
        return remote(
            pair_ref.at[:, pl.ds(r, size)],
            raw.at[pl.ds(pl.multiple_of(at.gz * c, c), c), pl.ds(r, size)],
            raw_send.at[t, side],
            raw_recv.at[lax.rem(t + side * half, chunks), at.gz],
            gz=nz // 2 - 1 + side,
        )

    def raw_wait(t, z):
        r = row_of(t, at.side)
        remote(
            pair_ref.at[:, pl.ds(r, size)],
            raw.at[pl.ds(pl.multiple_of(z * c, c), c), pl.ds(r, size)],
            raw_send.at[t, 0],
            raw_recv.at[lax.rem(t + at.side * half, chunks), z],
            gz=z,
        ).wait_recv()

    def weight_rows(index, z):
        return weight_ref.at[index, pl.ds(pl.multiple_of(z * h_z, h_z), h_z)]

    def weight_copy(index, side):
        return remote(
            given[index],
            weight_rows(index, at.gz),
            weight_send.at[side, index],
            weight_recv.at[at.gz, index],
            gz=nz // 2 - 1 + side,
        )

    def sends(stage, out_ref, block, send, recv, slot, r):
        first = pl.multiple_of(at.gy * block + r, size)
        where = (pl.ds(first, size), pl.ds(pl.multiple_of(at.gx * k, k), k))
        found = []
        for o in range(at.groups):
            q, qx, qy = at.member(o)
            src = stage.at[slot, pl.ds(q * per, near)]
            dst = out_ref.at[(pl.ds(0, near),) + where]
            if o == 0:
                found.append((pltpu.make_async_copy(src, dst, send.at[slot, 0]), True))
            else:
                found.append((remote(src, dst, send.at[slot, o], recv.at[at.group], gx=qx, gy=qy), False))
            if away:
                found.append(
                    (
                        remote(
                            stage.at[slot, pl.ds(q * per + near, away)],
                            out_ref.at[(pl.ds(0, away),) + where],
                            send.at[slot, at.groups + o],
                            recv.at[at.group],
                            gx=qx,
                            gy=qy,
                            gz=at.far,
                        ),
                        False,
                    )
                )
        return found

    def right_sends(t):
        return sends(
            right_stage, right_ref, rows, right_send, right_recv, lax.rem(t, SLOTS), row_of(t, at.side)
        )

    def left_sends(t):
        return sends(left_stage, left_ref, rows // 2, left_send, left_recv, lax.rem(t, SLOTS), t * size)

    def gate_copy(t):
        slot = lax.rem(t, 2)
        return pltpu.make_async_copy(
            gate_stage.at[slot], gate_ref.at[pl.ds(t * size, size)], gate_sem.at[slot]
        )

    def start(copies):
        for copy, _ in copies:
            copy.start()

    def drain(copies):
        for copy, is_local in copies:
            if is_local:
                copy.wait()
            else:
                copy.wait_send()

    def compute(t, with_left):
        slot = lax.rem(t, SLOTS)
        gate_slot = lax.rem(t, 2)
        r0 = row_of(t, at.side)
        gain = column(gain_ref[...])
        for g in range(size // GROUP):
            here = pl.ds(pl.multiple_of(r0 + g * GROUP, GROUP), GROUP)
            turn_in(
                raw_slab,
                lambda channel, part: raw[channel, here, part * LANES : (part + 1) * LANES],
                c_all,
            )

            def body(r, carry):
                row = r0 + g * GROUP + r
                normed = normalize(get_strided(raw_slab, r, c_all), gain)
                mask = mask_ref[pl.ds(row, 1), :].astype(jnp.float32)

                def part(index):
                    return jnp.dot(
                        weight_ref[index],
                        normed,
                        preferred_element_type=jnp.float32,
                    )

                put_strided(right_slab, r, mask * jax.nn.sigmoid(part(3)) * part(2))
                if with_left:
                    put_strided(left_slab, r, mask * jax.nn.sigmoid(part(1)) * part(0))
                    gate_stage[gate_slot, g * GROUP + r] = jax.nn.sigmoid(part(4)).astype(jnp.bfloat16)
                return carry

            lax.fori_loop(0, GROUP, body, 0)

            def stage_into(stage):
                def put(head, part, values):
                    stage[
                        slot,
                        head,
                        g * GROUP : (g + 1) * GROUP,
                        part * LANES : (part + 1) * LANES,
                    ] = values

                return put

            turn_out(right_slab, stage_into(right_stage), h)
            if with_left:
                turn_out(left_slab, stage_into(left_stage), h)

    def arrive(t):
        for o in range(1, nz):
            raw_wait(t, lax.rem(at.gz + o, nz))

    @pl.when(jnp.logical_not(at.is_mid))
    def _():
        def begin(t, carry):
            raw_copy(t, 0).start()
            raw_copy(t, 1).start()
            return carry

        for index in range(5):
            weight_copy(index, 0).start()
            weight_copy(index, 1).start()

        def end(t, carry):
            raw_copy(t, 0).wait_send()
            raw_copy(t, 1).wait_send()
            return carry

        lax.fori_loop(0, chunks, begin, 0)
        lax.fori_loop(0, chunks, end, 0)
        for index in range(5):
            weight_copy(index, 0).wait_send()
            weight_copy(index, 1).wait_send()

    @pl.when(at.is_mid)
    def _():
        other = 1 - at.side
        own = pltpu.make_async_copy(
            pair_ref, raw.at[pl.ds(pl.multiple_of(at.gz * c, c), c)], own_sem
        )
        own_weights = [
            pltpu.make_async_copy(
                given[index], weight_rows(index, at.gz), weight_recv.at[at.gz, index]
            )
            for index in range(5)
        ]
        for index in range(5):
            weight_copy(index, other).start()
            own_weights[index].start()
        own.start()
        for t in range(ahead):
            raw_copy(t, other).start()
        own.wait()
        for index in range(5):
            own_weights[index].wait()
            for o in range(1, nz):
                z = lax.rem(at.gz + o, nz)
                remote(
                    given[index],
                    weight_rows(index, z),
                    weight_send.at[0, index],
                    weight_recv.at[z, index],
                    gz=z,
                ).wait_recv()

        def step(t, with_left):
            @pl.when(t + ahead < chunks)
            def _():
                raw_copy(t + ahead, other).start()

            arrive(t)

            @pl.when(t >= SLOTS)
            def _():
                drain(right_sends(t - SLOTS))
                if with_left:
                    drain(left_sends(t - SLOTS))

            if with_left:

                @pl.when(t >= 2)
                def _():
                    gate_copy(t - 2).wait()

            compute(t, with_left)
            start(right_sends(t))
            if with_left:
                start(left_sends(t))
                gate_copy(t).start()

        def first(t, carry):
            step(t, True)
            return carry

        def second(t, carry):
            step(t, False)
            return carry

        lax.fori_loop(0, half, first, 0)
        lax.fori_loop(half, chunks, second, 0)
        for t in range(max(half - 2, 0), half):
            gate_copy(t).wait()
        for t in range(max(half - SLOTS, 0), half):
            drain(left_sends(t))
        for t in range(max(chunks - SLOTS, 0), chunks):
            drain(right_sends(t))

        def end(t, carry):
            raw_copy(t, other).wait_send()
            return carry

        lax.fori_loop(0, chunks, end, 0)
        for index in range(5):
            weight_copy(index, other).wait_send()

    def collect(heads, first_offset):
        for o in range(first_offset, at.groups):
            q, qx, qy = at.member(o)
            for out_ref, block, recv in (
                (right_ref, rows, right_recv),
                (left_ref, rows // 2, left_recv),
            ):
                whole = out_ref.at[
                    pl.ds(0, heads),
                    pl.ds(pl.multiple_of(qy * block, block), block),
                    pl.ds(pl.multiple_of(qx * k, k), k),
                ]
                remote(whole, whole, own_sem, recv.at[q], gz=at.mid).wait_recv()

    @pl.when(at.is_mid)
    def _():
        collect(near, 1)

    if away:

        @pl.when(at.is_far)
        def _():
            collect(away, 0)


def mix_kernel(
    dims,
    right_ref,
    left_ref,
    gate_ref,
    gain_part_ref,
    w_out_ref,
    out_ref,
    right,
    left,
    stage,
    mix,
    gate,
    out_stage,
    gains_ref,
    gain_ref,
    weight_ref,
    in_slab,
    out_slab,
    weight_send,
    weight_recv,
    right_sem,
    left_sem,
    gate_sem,
    mix_send,
    mix_recv,
    out_send,
    out_recv,
):
    nx, ny, nz, near, away = dims
    at = Place(nx, ny, nz)
    c, rows, k = out_ref.shape
    c_z, h = w_out_ref.shape
    h_z = gain_part_ref.shape[1]
    own_rows = rows // 2
    steps = own_rows // GROUP
    per = near + away
    deep = max(near, away)

    def left_copies(t, heads):
        slot = lax.rem(t, 2)
        return [
            pltpu.make_async_copy(
                left_ref.at[pl.ds(0, heads), pl.ds(pl.multiple_of(y * own_rows + t * GROUP, GROUP), GROUP)],
                left.at[slot, pl.ds(0, heads), pl.ds(y * GROUP, GROUP)],
                left_sem.at[slot, y],
            )
            for y in range(ny)
        ]

    def right_copy(head):
        return pltpu.make_async_copy(right_ref.at[head], right.at[head], right_sem.at[head])

    def gate_copy(t):
        slot = lax.rem(t, 2)
        return pltpu.make_async_copy(
            gate_ref.at[pl.ds(t * GROUP, GROUP)], gate.at[slot], gate_sem.at[slot]
        )

    def mix_sends(t, heads, shift, first_offset):
        slot = lax.rem(t, SLOTS)
        found = []
        for o in range(first_offset, at.groups):
            q, qx, qy = at.member(o)
            found.append(
                remote(
                    stage.at[
                        slot,
                        pl.ds(0, heads),
                        pl.ds(pl.multiple_of(qy * GROUP, GROUP), GROUP),
                        pl.ds(pl.multiple_of(qx * k, k), k),
                    ],
                    mix.at[
                        pl.ds(at.group * per + shift, heads),
                        pl.ds(pl.multiple_of(t * GROUP, GROUP), GROUP),
                    ],
                    mix_send.at[slot, o],
                    mix_recv.at[t],
                    gx=qx,
                    gy=qy,
                    gz=at.mid,
                )
            )
        return found

    def multiply(t, heads, shift, first_offset):
        slot = lax.rem(t, SLOTS)
        left_slot = lax.rem(t, 2)

        @pl.when(t + 1 < steps)
        def _():
            for copy in left_copies(t + 1, heads):
                copy.start()

        for copy in left_copies(t, heads):
            copy.wait()

        @pl.when(t >= SLOTS)
        def _():
            for copy in mix_sends(t - SLOTS, heads, shift, first_offset):
                copy.wait_send()

        def body(head, carry):
            @pl.when(t == 0)
            def _():
                right_copy(head).wait()

            product = lax.dot_general(
                left[left_slot, head],
                right[head],
                (((1,), (1,)), ((), ())),
                preferred_element_type=jnp.float32,
            )
            stage[slot, head] = product.astype(jnp.bfloat16)
            return carry

        lax.fori_loop(0, heads, body, 0)
        for copy in mix_sends(t, heads, shift, first_offset):
            copy.start()

    def begin(heads):
        for copy in left_copies(0, heads):
            copy.start()
        for head in range(heads):
            right_copy(head).start()

    def end(heads, shift, first_offset):
        for t in range(max(steps - SLOTS, 0), steps):
            for copy in mix_sends(t, heads, shift, first_offset):
                copy.wait_send()

    def out_copies(t):
        slot = lax.rem(t, SLOTS)
        where = pl.ds(pl.multiple_of(at.side * own_rows + t * GROUP, GROUP), GROUP)
        found = [
            (
                pltpu.make_async_copy(
                    out_stage.at[slot, pl.ds(pl.multiple_of(at.gz * c, c), c)],
                    out_ref.at[:, where],
                    out_send.at[slot, 0],
                ),
                True,
            )
        ]
        for o in range(1, nz):
            z = lax.rem(at.gz + o, nz)
            found.append(
                (
                    remote(
                        out_stage.at[slot, pl.ds(pl.multiple_of(z * c, c), c)],
                        out_ref.at[:, where],
                        out_send.at[slot, o],
                        out_recv.at[at.side],
                        gz=z,
                    ),
                    False,
                )
            )
        return found

    def drain_out(t):
        for copy, is_local in out_copies(t):
            if is_local:
                copy.wait()
            else:
                copy.wait_send()

    def finish(t):
        slot = lax.rem(t, SLOTS)
        gate_slot = lax.rem(t, 2)
        here = pl.ds(pl.multiple_of(t * GROUP, GROUP), GROUP)
        if h > near:
            rest = mix.at[pl.ds(0, h - near), here]
            remote(rest, rest, out_send.at[0, 0], mix_recv.at[t], gz=at.mid).wait_recv()

        gain = gain_ref[...]
        turn_in(
            in_slab,
            lambda head, part: mix[head, here, part * LANES : (part + 1) * LANES],
            h,
        )

        @pl.when(t + 1 < steps)
        def _():
            gate_copy(t + 1).start()

        gate_copy(t).wait()

        def body(r, carry):
            normed = normalize(get_strided(in_slab, r, h), gain)
            projected = jnp.dot(weight_ref[...], normed, preferred_element_type=jnp.float32)
            put_strided(out_slab, r, gate[gate_slot, r].astype(jnp.float32) * projected)
            return carry

        lax.fori_loop(0, GROUP, body, 0)

        @pl.when(t >= SLOTS)
        def _():
            drain_out(t - SLOTS)

        def put(head, part, values):
            out_stage[slot, head, :, part * LANES : (part + 1) * LANES] = values

        turn_out(out_slab, put, c * nz)
        for copy, _ in out_copies(t):
            copy.start()

    lag = min(LAG, steps)

    def small(z):
        return (
            (gain_part_ref, gains_ref.at[z]),
            (w_out_ref, weight_ref.at[pl.ds(pl.multiple_of(z * c_z, c_z), c_z)]),
        )

    def weight_copies(side):
        return [
            remote(
                src,
                dst,
                weight_send.at[side, index],
                weight_recv.at[at.gz, index],
                gz=nz // 2 - 1 + side,
            )
            for index, (src, dst) in enumerate(small(at.gz))
        ]

    def own_weights():
        return [
            pltpu.make_async_copy(src, dst, weight_recv.at[at.gz, index])
            for index, (src, dst) in enumerate(small(at.gz))
        ]

    def take_weights():
        for copy in own_weights():
            copy.wait()
        for o in range(1, nz):
            z = lax.rem(at.gz + o, nz)
            for index, (src, dst) in enumerate(small(z)):
                remote(
                    src, dst, weight_send.at[0, index], weight_recv.at[z, index], gz=z
                ).wait_recv()
        for z in range(nz):
            gain_ref[z * h_z : (z + 1) * h_z, :] = column(gains_ref[z])

    @pl.when(jnp.logical_not(at.is_mid))
    def _():
        for side in range(2):
            for copy in weight_copies(side):
                copy.start()
        for side in range(2):
            for copy in weight_copies(side):
                copy.wait_send()

    @pl.when(at.is_mid)
    def _():
        for copy in weight_copies(1 - at.side):
            copy.start()
        for copy in own_weights():
            copy.start()
        begin(near)
        gate_copy(0).start()

        def keep_own(t):
            slot = lax.rem(t, SLOTS)
            mix[
                pl.ds(at.group * per, near), pl.ds(pl.multiple_of(t * GROUP, GROUP), GROUP)
            ] = stage[
                slot,
                0:near,
                pl.ds(pl.multiple_of(at.gy * GROUP, GROUP), GROUP),
                pl.ds(pl.multiple_of(at.gx * k, k), k),
            ]

        def step(t, carry):
            multiply(t, near, 0, 1)
            keep_own(t)

            @pl.when(t == lag)
            def _():
                take_weights()

            @pl.when(t >= lag)
            def _():
                finish(t - lag)

            return carry

        def last(t, carry):
            finish(t)
            return carry

        lax.fori_loop(0, steps, step, 0)
        if lag >= steps:
            take_weights()
        lax.fori_loop(steps - lag, steps, last, 0)
        end(near, 0, 1)
        for t in range(max(steps - SLOTS, 0), steps):
            drain_out(t)
        for copy in weight_copies(1 - at.side):
            copy.wait_send()

    if away:

        @pl.when(at.is_far)
        def _():
            begin(away)

            def step(t, carry):
                multiply(t, away, near, 0)
                return carry

            lax.fori_loop(0, steps, step, 0)
            end(away, near, 0)

    for side in range(2):
        source = nz // 2 - 1 + side

        @pl.when(at.gz != source)
        def _():
            where = out_ref.at[:, pl.ds(side * own_rows, own_rows)]
            remote(where, where, out_send.at[0, 0], out_recv.at[side], gz=source).wait_recv()


def local(
    pair,
    pair_mask,
    in_gain,
    w_left,
    w_left_gate,
    w_right,
    w_right_gate,
    w_out_gate,
    out_gain,
    w_out,
):
    nx, ny, nz = (lax.axis_size(a) for a in ("gx", "gy", "gz"))
    c, rows, k = pair.shape
    c_all = c * nz
    h = w_left.shape[1] * nz
    groups = nx * ny
    per = h // groups
    away = 0 if nz < 4 else max(1, per * 5 // 16)
    near = per - away
    deep = max(near, away)
    dims = (nx, ny, nz, near, away)
    size = min(GROUP, rows // 2)
    chunks = rows // size
    steps = rows // 2 // GROUP
    parts = k // LANES

    anywhere = pl.BlockSpec(memory_space=pl.ANY)
    vmem = pl.BlockSpec(memory_space=pltpu.VMEM)
    bf16 = lambda *shape: jax.ShapeDtypeStruct(shape, jnp.bfloat16)
    sem = pltpu.SemaphoreType.DMA
    slab = pltpu.VMEM((parts, h * PITCH, LANES), jnp.float32)
    params = pltpu.CompilerParams(has_side_effects=True, vmem_limit_bytes=VMEM_LIMIT)

    right, left, gate = pl.pallas_call(
        functools.partial(project_kernel, dims),
        out_shape=(
            bf16(deep, ny * rows, nx * k),
            bf16(deep, ny * rows // 2, nx * k),
            bf16(rows // 2, h, k),
        ),
        in_specs=[anywhere, vmem, vmem] + [anywhere] * 5,
        out_specs=(anywhere, anywhere, anywhere),
        scratch_shapes=[
            pltpu.VMEM((c_all, rows, k), jnp.bfloat16),
            pltpu.VMEM((5, h, c_all), jnp.bfloat16),
            pltpu.VMEM((SLOTS, h, size, k), jnp.bfloat16),
            pltpu.VMEM((SLOTS, h, size, k), jnp.bfloat16),
            pltpu.VMEM((2, size, h, k), jnp.bfloat16),
            pltpu.VMEM((parts, c_all * PITCH, LANES), jnp.float32),
            slab,
            slab,
            sem((chunks, 2)),
            sem((chunks, nz)),
            sem((2, 5)),
            sem((nz, 5)),
            sem,
            sem((SLOTS, 2 * groups)),
            sem((SLOTS, 2 * groups)),
            sem((groups,)),
            sem((groups,)),
            sem((2,)),
        ],
        compiler_params=params,
    )(
        pair,
        pair_mask,
        in_gain[None, :],
        w_left.T,
        w_left_gate.T,
        w_right.T,
        w_right_gate.T,
        w_out_gate.T,
    )

    return pl.pallas_call(
        functools.partial(mix_kernel, dims),
        out_shape=bf16(c, rows, k),
        in_specs=[anywhere] * 5,
        out_specs=anywhere,
        scratch_shapes=[
            pltpu.VMEM((deep, ny * rows, nx * k), jnp.bfloat16),
            pltpu.VMEM((2, deep, ny * GROUP, nx * k), jnp.bfloat16),
            pltpu.VMEM((SLOTS, deep, ny * GROUP, ny * rows), jnp.bfloat16),
            pltpu.VMEM((h, rows // 2, k), jnp.bfloat16),
            pltpu.VMEM((2, GROUP, h, k), jnp.bfloat16),
            pltpu.VMEM((SLOTS, c_all, GROUP, k), jnp.bfloat16),
            pltpu.VMEM((nz, 1, h // nz), jnp.float32),
            pltpu.VMEM((h, 1), jnp.float32),
            pltpu.VMEM((c_all, h), jnp.bfloat16),
            slab,
            pltpu.VMEM((parts, c_all * PITCH, LANES), jnp.float32),
            sem((2, 2)),
            sem((nz, 2)),
            sem((deep,)),
            sem((2, ny)),
            sem((2,)),
            sem((SLOTS, groups)),
            sem((steps,)),
            sem((SLOTS, nz)),
            sem((2,)),
        ],
        compiler_params=params,
    )(right, left, gate, out_gain[None, :], w_out.T)


def solution(mesh):
    placed = (
        P("gz", "gy", "gx"),
        P("gy", "gx"),
        P(),
        P(None, "gz"),
        P(None, "gz"),
        P(None, "gz"),
        P(None, "gz"),
        P(None, "gz"),
        P("gz"),
        P(None, "gz"),
    )
    return jax.shard_map(
        local, mesh=mesh, in_specs=placed, out_specs=P("gz", "gy", "gx"), check_vma=False
    )
```

```python
import functools

import jax
import jax.numpy as jnp
from jax import lax
from jax.experimental import pallas as pl
from jax.experimental.pallas import tpu as pltpu
from jax.sharding import PartitionSpec as P

epsilon = 1e-05
MESH = pl.DeviceIdType.MESH
LANES = 128
GROUP = 16
PITCH = GROUP + 1
SLOTS = 4
LAG = 2
WIDE = 2
VMEM_LIMIT = 67043328


def normalize(values, gain):
    average = jnp.mean(values, axis=0, keepdims=True)
    centered = values - average
    spread = jnp.mean(jnp.square(centered), axis=0, keepdims=True)
    return (centered * lax.rsqrt(spread + epsilon) * gain).astype(jnp.bfloat16)


class Place:
    def __init__(self, nx, ny, nz):
        self.nx, self.ny, self.nz = nx, ny, nz
        self.gx, self.gy, self.gz = (lax.axis_index(a) for a in ("gx", "gy", "gz"))
        self.group = self.gx * ny + self.gy
        self.groups = nx * ny
        self.side = self.gz // (nz // 2)
        self.mid = nz // 2 - 1 + self.side
        self.far = self.side * (nz - 1)
        self.is_mid = self.gz == self.mid
        self.is_far = jnp.logical_and(self.gz == self.far, jnp.logical_not(self.is_mid))

    def member(self, offset):
        q = lax.rem(self.group + offset, self.groups)
        return q, q // self.ny, lax.rem(q, self.ny)


def block(start, size):
    return pl.ds(pl.multiple_of(start, size), size)


def remote(src, dst, send, recv, **device):
    return pltpu.make_async_remote_copy(
        src_ref=src, dst_ref=dst, send_sem=send, recv_sem=recv, device_id=device, device_id_type=MESH
    )


def column(row):
    n = row.shape[1]
    same = lax.broadcasted_iota(jnp.int32, (n, n), 0) == lax.broadcasted_iota(jnp.int32, (n, n), 1)
    return jnp.sum(jnp.where(same, row, 0.0), axis=1, keepdims=True)


def turn_in(slab, source, count):
    def body(i, carry):
        for u in range(8):
            channel = i * 8 + u
            for part in range(slab.shape[0]):
                slab.at[part][pl.ds(channel * PITCH, GROUP), :] = source(channel, part).astype(
                    jnp.float32
                )
        return carry

    lax.fori_loop(0, count // 8, body, 0)


def turn_out(slab, put, count):
    def body(i, carry):
        for u in range(8):
            channel = i * 8 + u
            for part in range(slab.shape[0]):
                rows = slab.at[part][pl.ds(channel * PITCH, GROUP), :]
                put(channel, part, rows.astype(jnp.bfloat16))
        return carry

    lax.fori_loop(0, count // 8, body, 0)


def get_rows(slab, row, count):
    return jnp.concatenate(
        [
            slab.at[part][pl.ds(row + u, count, stride=PITCH), :]
            for u in range(WIDE)
            for part in range(slab.shape[0])
        ],
        axis=1,
    )


def put_rows(slab, row, values):
    parts = slab.shape[0]
    for u in range(WIDE):
        for part in range(parts):
            lane = (u * parts + part) * LANES
            slab.at[part][pl.ds(row + u, values.shape[0], stride=PITCH), :] = values[
                :, lane : lane + LANES
            ]


def start(copies):
    for copy, _ in copies:
        copy.start()


def drain(copies):
    for copy, is_local in copies:
        if is_local:
            copy.wait()
        else:
            copy.wait_send()


def update_kernel(
    dims,
    pair_ref,
    mask_ref,
    gain_row_ref,
    mix_gain_ref,
    w0_ref,
    w1_ref,
    w2_ref,
    w3_ref,
    w4_ref,
    w5_ref,
    out_ref,
    raw_ref,
    left_ref,
    gate_ref,
    right,
    mix,
    ring,
    left,
    right_stage,
    left_stage,
    gate_stage,
    mix_stage,
    in_slab,
    out_slab,
    left_slab,
    weight,
    mix_weight,
    mix_gain_parts,
    mix_gain,
    raw_send,
    raw_recv,
    load_sem,
    small_send,
    small_recv,
    right_send,
    left_send,
    right_recv,
    left_recv,
    gate_sem,
    left_sem,
    mix_send,
    mix_recv,
    out_send,
    out_recv,
    credit,
):
    nx, ny, nz, near, away = dims
    at = Place(nx, ny, nz)
    c, rows, k = pair_ref.shape
    h_z, c_all = w0_ref.shape
    h = h_z * nz
    chunks = rows // GROUP
    half = chunks // 2
    own_rows = rows // 2
    steps = half
    per = near + away
    ahead = min(6, chunks)
    lag = min(LAG, steps)
    parts = k // LANES
    other = 1 - at.side

    def mid_of(side):
        return nz // 2 - 1 + side


    def chunk_of(t, side):
        return lax.rem(t + side * half, chunks)

    def raw_copy(t, side):
        chunk = chunk_of(t, side)
        where = block(chunk * GROUP, GROUP)
        return remote(
            pair_ref.at[:, where],
            raw_ref.at[block(at.gz * c, c), where],
            raw_send.at[t, side],
            raw_recv.at[chunk, at.gz],
            gz=mid_of(side),
        )

    def arrive(t):
        chunk = chunk_of(t, at.side)
        where = block(chunk * GROUP, GROUP)
        for o in range(1, nz):
            z = lax.rem(at.gz + o, nz)
            landed = raw_ref.at[block(z * c, c), where]
            remote(landed, landed, raw_send.at[t, 0], raw_recv.at[chunk, z], gz=z).wait_recv()

    def loads(t):
        slot = lax.rem(t, 2)
        where = block(chunk_of(t, at.side) * GROUP, GROUP)
        found = []
        for o in range(nz):
            z = lax.rem(at.gz + o, nz)
            src = pair_ref.at[:, where] if o == 0 else raw_ref.at[block(z * c, c), where]
            found.append(
                pltpu.make_async_copy(src, ring.at[slot, block(z * c, c)], load_sem.at[slot, o])
            )
        return found

    def small(z):
        sources = (w0_ref, w1_ref, w2_ref, w3_ref, w4_ref)
        found = [(src, weight.at[index, block(z * h_z, h_z)]) for index, src in enumerate(sources)]
        found.append((w5_ref, mix_weight.at[block(z * c, c)]))
        found.append((mix_gain_ref, mix_gain_parts.at[z]))
        return list(enumerate(found))

    def small_copies(side):
        return [
            (
                remote(
                    src, dst, small_send.at[side, i], small_recv.at[at.gz, i], gz=mid_of(side)
                ),
                False,
            )
            for i, (src, dst) in small(at.gz)
        ]

    def small_own():
        return [
            (pltpu.make_async_copy(src, dst, small_recv.at[at.gz, i]), True)
            for i, (src, dst) in small(at.gz)
        ]

    def small_arrive():
        drain(small_own())
        for o in range(1, nz):
            z = lax.rem(at.gz + o, nz)
            for i, (src, dst) in small(z):
                remote(src, dst, small_send.at[0, i], small_recv.at[z, i], gz=z).wait_recv()
        for z in range(nz):
            mix_gain[z * h_z : (z + 1) * h_z, :] = column(mix_gain_parts[z])


    def sends(stage, out, first, send, recv, slot):
        where = (block(first, GROUP), block(at.gx * k, k))
        found = []
        for o in range(at.groups):
            q, qx, qy = at.member(o)
            if o > 0:
                found.append(
                    (
                        remote(
                            stage.at[slot, pl.ds(q * per, near)],
                            out.at[(pl.ds(0, near),) + where],
                            send.at[slot, o],
                            recv.at[at.group],
                            gx=qx,
                            gy=qy,
                        ),
                        False,
                    )
                )
            if away:
                found.append(
                    (
                        remote(
                            stage.at[slot, pl.ds(q * per + near, away)],
                            out.at[(pl.ds(0, away),) + where],
                            send.at[slot, at.groups + o],
                            recv.at[at.group],
                            gx=qx,
                            gy=qy,
                            gz=at.far,
                        ),
                        False,
                    )
                )
        return found

    def right_first(t):
        return at.gy * rows + chunk_of(t, at.side) * GROUP

    def left_first(t):
        return at.gy * own_rows + t * GROUP

    def right_sends(t):
        slot = lax.rem(t, SLOTS)
        return sends(right_stage, right, right_first(t), right_send, right_recv, slot)

    def left_sends(t):
        slot = lax.rem(t, SLOTS)
        own = pltpu.make_async_copy(
            left_stage.at[slot, pl.ds(at.group * per, near)],
            left_ref.at[pl.ds(0, near), block(left_first(t), GROUP), block(at.gx * k, k)],
            left_send.at[slot, 0],
        )
        return sends(left_stage, left_ref, left_first(t), left_send, left_recv, slot) + [(own, True)]

    def gate_out(t):
        slot = lax.rem(t, 2)
        return pltpu.make_async_copy(
            gate_stage.at[slot], gate_ref.at[pl.ds(t * GROUP, GROUP)], gate_sem.at[slot]
        )

    def project(t, with_left):
        slot = lax.rem(t, SLOTS)
        gate_slot = lax.rem(t, 2)
        load_slot = lax.rem(t, 2)
        r0 = chunk_of(t, at.side) * GROUP
        gain = column(gain_row_ref[...])
        turn_in(
            in_slab,
            lambda channel, part: ring[load_slot, channel, :, part * LANES : (part + 1) * LANES],
            c_all,
        )

        def body(i, carry):
            r = i * WIDE
            normed = normalize(get_rows(in_slab, r, c_all), gain)
            mask = jnp.concatenate(
                [mask_ref[pl.ds(r0 + r + u, 1), :] for u in range(WIDE)], axis=1
            ).astype(jnp.float32)

            def part(index):
                return jnp.dot(weight[index], normed, preferred_element_type=jnp.float32)

            put_rows(out_slab, r, mask * jax.nn.sigmoid(part(3)) * part(2))
            if with_left:
                put_rows(left_slab, r, mask * jax.nn.sigmoid(part(1)) * part(0))
                gates = jax.nn.sigmoid(part(4)).astype(jnp.bfloat16)
                for u in range(WIDE):
                    gate_stage[gate_slot, r + u] = gates[:, u * k : (u + 1) * k]
            return carry

        lax.fori_loop(0, GROUP // WIDE, body, 0)

        def stage_into(stage):
            def put(head, part, values):
                stage[slot, head, :, part * LANES : (part + 1) * LANES] = values

            return put

        turn_out(out_slab, stage_into(right_stage), h)
        right[0:near, block(right_first(t), GROUP), block(at.gx * k, k)] = right_stage[
            slot, pl.ds(at.group * per, near)
        ]
        if with_left:
            turn_out(left_slab, stage_into(left_stage), h)

    def collect(heads, first_offset):
        for o in range(first_offset, at.groups):
            q, qx, qy = at.member(o)
            for out, size, recv in ((right, rows, right_recv), (left_ref, own_rows, left_recv)):
                whole = out.at[pl.ds(0, heads), block(qy * size, size), block(qx * k, k)]
                remote(whole, whole, gate_sem.at[0], recv.at[q], gz=at.mid).wait_recv()


    def left_loads(t, heads):
        slot = lax.rem(t, 2)
        return [
            pltpu.make_async_copy(
                left_ref.at[pl.ds(0, heads), block(y * own_rows + t * GROUP, GROUP)],
                left.at[slot, pl.ds(0, heads), pl.ds(y * GROUP, GROUP)],
                left_sem.at[slot, y],
            )
            for y in range(ny)
        ]

    def mix_sends(t, heads, shift, first_offset):
        slot = lax.rem(t, SLOTS)
        found = []
        for o in range(first_offset, at.groups):
            q, qx, qy = at.member(o)
            found.append(
                (
                    remote(
                        mix_stage.at[
                            slot, pl.ds(0, heads), block(qy * GROUP, GROUP), block(qx * k, k)
                        ],
                        mix.at[pl.ds(at.group * per + shift, heads), block(t * GROUP, GROUP)],
                        mix_send.at[slot, o],
                        mix_recv.at[t],
                        gx=qx,
                        gy=qy,
                        gz=at.mid,
                    ),
                    False,
                )
            )
        return found

    def multiply(t, heads, shift, first_offset, paced=False):
        slot = lax.rem(t, SLOTS)
        left_slot = lax.rem(t, 2)

        @pl.when(t + 1 < steps)
        def _():
            for copy in left_loads(t + 1, heads):
                copy.start()

        for copy in left_loads(t, heads):
            copy.wait()

        @pl.when(t >= SLOTS)
        def _():
            drain(mix_sends(t - SLOTS, heads, shift, first_offset))

        def body(head, carry):
            product = lax.dot_general(
                left[left_slot, head],
                right[head],
                (((1,), (1,)), ((), ())),
                preferred_element_type=jnp.float32,
            )
            mix_stage[slot, head] = product.astype(jnp.bfloat16)
            return carry

        lax.fori_loop(0, heads, body, 0)
        if paced:

            @pl.when(t >= 1)
            def _():
                pl.semaphore_wait(credit, 1)

        start(mix_sends(t, heads, shift, first_offset))

    def multiply_end(heads, shift, first_offset):
        for t in range(max(steps - SLOTS, 0), steps):
            drain(mix_sends(t, heads, shift, first_offset))


    def gate_load(t):
        slot = lax.rem(t, 2)
        return pltpu.make_async_copy(
            gate_ref.at[pl.ds(t * GROUP, GROUP)], gate_stage.at[slot], gate_sem.at[slot]
        )

    def out_copies(t):
        slot = lax.rem(t, SLOTS)
        where = block(at.side * own_rows + t * GROUP, GROUP)
        own = pltpu.make_async_copy(
            right_stage.at[slot, block(at.gz * c, c)], out_ref.at[:, where], out_send.at[slot, 0]
        )
        found = [(own, True)]
        for o in range(1, nz):
            z = lax.rem(at.gz + o, nz)
            found.append(
                (
                    remote(
                        right_stage.at[slot, block(z * c, c)],
                        out_ref.at[:, where],
                        out_send.at[slot, o],
                        out_recv.at[at.side],
                        gz=z,
                    ),
                    False,
                )
            )
        return found

    def finish(t):
        slot = lax.rem(t, SLOTS)
        gate_slot = lax.rem(t, 2)
        here = block(t * GROUP, GROUP)
        if h > near:
            rest = mix.at[pl.ds(0, h - near), here]
            remote(rest, rest, out_send.at[0, 0], mix_recv.at[t], gz=at.mid).wait_recv()

        gain = mix_gain[...]
        turn_in(
            in_slab, lambda head, part: mix[head, here, part * LANES : (part + 1) * LANES], h
        )

        @pl.when(t + 1 < steps)
        def _():
            gate_load(t + 1).start()

        gate_load(t).wait()

        def body(i, carry):
            r = i * WIDE
            normed = normalize(get_rows(in_slab, r, h), gain)
            projected = jnp.dot(mix_weight[...], normed, preferred_element_type=jnp.float32)
            gates = jnp.concatenate([gate_stage[gate_slot, r + u] for u in range(WIDE)], axis=1)
            put_rows(out_slab, r, gates.astype(jnp.float32) * projected)
            return carry

        lax.fori_loop(0, GROUP // WIDE, body, 0)

        @pl.when(t >= SLOTS)
        def _():
            drain(out_copies(t - SLOTS))

        def put(channel, part, values):
            right_stage[slot, channel, :, part * LANES : (part + 1) * LANES] = values

        turn_out(out_slab, put, c_all)
        start(out_copies(t))


    @pl.when(jnp.logical_not(at.is_mid))
    def _():
        def begin(t, carry):
            raw_copy(t, 0).start()
            raw_copy(t, 1).start()
            return carry

        def end(t, carry):
            raw_copy(t, 0).wait_send()
            raw_copy(t, 1).wait_send()
            return carry

        for side in range(2):
            start(small_copies(side))
        lax.fori_loop(0, chunks, begin, 0)
        lax.fori_loop(0, chunks, end, 0)
        for side in range(2):
            drain(small_copies(side))

    if away:

        @pl.when(at.is_far)
        def _():
            collect(away, 0)
            for copy in left_loads(0, away):
                copy.start()

            def step(t, carry):
                multiply(t, away, near, 0, True)
                return carry

            lax.fori_loop(0, steps, step, 0)
            multiply_end(away, near, 0)

    @pl.when(at.is_mid)
    def _():
        start(small_own())
        start(small_copies(other))
        for t in range(ahead):
            raw_copy(t, other).start()
        small_arrive()
        arrive(0)
        for copy in loads(0):
            copy.start()

        def step(t, with_left):
            @pl.when(t + ahead < chunks)
            def _():
                raw_copy(t + ahead, other).start()

            @pl.when(t >= SLOTS)
            def _():
                drain(right_sends(t - SLOTS))
                if with_left:
                    drain(left_sends(t - SLOTS))

            if with_left:

                @pl.when(t >= 2)
                def _():
                    gate_out(t - 2).wait()

            for copy in loads(t):
                copy.wait()
            project(t, with_left)
            start(right_sends(t))
            if with_left:
                start(left_sends(t))
                gate_out(t).start()

            @pl.when(t + 1 < chunks)
            def _():
                arrive(t + 1)
                for copy in loads(t + 1):
                    copy.start()

        def first(t, carry):
            step(t, True)
            return carry

        def second(t, carry):
            step(t, False)
            return carry

        lax.fori_loop(0, half, first, 0)
        for t in range(max(half - 2, 0), half):
            gate_out(jnp.int32(t)).wait()
        gate_load(jnp.int32(0)).start()
        lax.fori_loop(half, chunks, second, 0)
        for t in range(max(half - SLOTS, 0), half):
            drain(left_sends(t))
        for t in range(max(chunks - SLOTS, 0), chunks):
            drain(right_sends(t))
        collect(near, 1)
        for copy in left_loads(0, near):
            copy.start()

        def both(t, carry):
            multiply(t, near, 0, 1)
            if away:

                @pl.when(t + 1 < steps)
                def _():
                    pl.semaphore_signal(
                        credit, inc=1, device_id={"gz": at.far}, device_id_type=MESH
                    )

            slot = lax.rem(t, SLOTS)
            mix[pl.ds(at.group * per, near), block(t * GROUP, GROUP)] = mix_stage[
                slot, 0:near, block(at.gy * GROUP, GROUP), block(at.gx * k, k)
            ]

            @pl.when(t >= lag)
            def _():
                finish(t - lag)

            return carry

        def last(t, carry):
            finish(t)
            return carry

        lax.fori_loop(0, steps, both, 0)
        lax.fori_loop(steps - lag, steps, last, 0)
        multiply_end(near, 0, 1)
        for t in range(max(steps - SLOTS, 0), steps):
            drain(out_copies(t))
        drain(small_copies(other))

        def end(t, carry):
            raw_copy(t, other).wait_send()
            return carry

        lax.fori_loop(0, chunks, end, 0)

    for side in range(2):

        @pl.when(at.gz != mid_of(side))
        def _():
            where = out_ref.at[:, pl.ds(side * own_rows, own_rows)]
            remote(where, where, gate_sem.at[0], out_recv.at[side], gz=mid_of(side)).wait_recv()


def local(
    pair,
    pair_mask,
    in_gain,
    w_left,
    w_left_gate,
    w_right,
    w_right_gate,
    w_out_gate,
    out_gain,
    w_out,
):
    nx, ny, nz = (lax.axis_size(a) for a in ("gx", "gy", "gz"))
    c, rows, k = pair.shape
    c_all = c * nz
    h = w_left.shape[1] * nz
    groups = nx * ny
    per = h // groups
    away = 0 if nz < 4 else max(1, per * 5 // 16)
    near = per - away
    deep = max(near, away)
    dims = (nx, ny, nz, near, away)
    chunks = rows // GROUP
    steps = chunks // 2
    parts = k // LANES
    widest = max(h, c_all)

    anywhere = pl.BlockSpec(memory_space=pl.ANY)
    whole = pl.BlockSpec(memory_space=pltpu.VMEM)
    shape = lambda *dims: jax.ShapeDtypeStruct(dims, jnp.bfloat16)
    half = lambda *dims: pltpu.VMEM(dims, jnp.bfloat16)
    full = lambda *dims: pltpu.VMEM(dims, jnp.float32)
    sem = pltpu.SemaphoreType.DMA

    return pl.pallas_call(
        functools.partial(update_kernel, dims),
        out_shape=(
            shape(c, rows, k),
            shape(c_all, rows, k),
            shape(deep, ny * rows // 2, nx * k),
            shape(rows // 2, h, k),
        ),
        in_specs=[anywhere, whole, whole] + [anywhere] * 7,
        out_specs=(anywhere,) * 4,
        scratch_shapes=[
            half(deep, ny * rows, nx * k),
            half(h, rows // 2, k),
            half(2, c_all, GROUP, k),
            half(2, deep, ny * GROUP, nx * k),
            half(SLOTS, widest, GROUP, k),
            half(SLOTS, h, GROUP, k),
            half(2, GROUP, h, k),
            half(SLOTS, deep, ny * GROUP, ny * rows),
            full(parts, widest * PITCH, LANES),
            full(parts, widest * PITCH, LANES),
            full(parts, h * PITCH, LANES),
            half(5, h, c_all),
            half(c_all, h),
            full(nz, 1, h // nz),
            full(h, 1),
            sem((chunks, 2)),
            sem((chunks, nz)),
            sem((2, nz)),
            sem((2, 7)),
            sem((nz, 7)),
            sem((SLOTS, 2 * groups)),
            sem((SLOTS, 2 * groups)),
            sem((groups,)),
            sem((groups,)),
            sem((2,)),
            sem((2, ny)),
            sem((SLOTS, groups)),
            sem((steps,)),
            sem((SLOTS, nz)),
            sem((2,)),
            pltpu.SemaphoreType.REGULAR,
        ],
        compiler_params=pltpu.CompilerParams(has_side_effects=True, vmem_limit_bytes=VMEM_LIMIT),
    )(
        pair,
        pair_mask,
        in_gain[None, :],
        out_gain[None, :],
        w_left.T,
        w_left_gate.T,
        w_right.T,
        w_right_gate.T,
        w_out_gate.T,
        w_out.T,
    )[0]


def solution(mesh):
    placed = (
        P("gz", "gy", "gx"),
        P("gy", "gx"),
        P(),
        P(None, "gz"),
        P(None, "gz"),
        P(None, "gz"),
        P(None, "gz"),
        P(None, "gz"),
        P("gz"),
        P(None, "gz"),
    )
    return jax.shard_map(
        local, mesh=mesh, in_specs=placed, out_specs=P("gz", "gy", "gx"), check_vma=False
    )
```

```python
import functools

import jax
import jax.numpy as jnp
from jax import lax
from jax.experimental import pallas as pl
from jax.experimental.pallas import tpu as pltpu
from jax.sharding import PartitionSpec as P

epsilon = 1e-05
MESH = pl.DeviceIdType.MESH
LANES = 128
GROUP = 16
PITCH = GROUP + 1
SLOTS = 4
LAG = 2
WIDE = 2
VMEM_LIMIT = 67043328


def normalize(values, gain):
    average = jnp.mean(values, axis=0, keepdims=True)
    centered = values - average
    spread = jnp.mean(jnp.square(centered), axis=0, keepdims=True)
    return (centered * lax.rsqrt(spread + epsilon) * gain).astype(jnp.bfloat16)


class Place:
    def __init__(self, nx, ny, nz):
        self.nx, self.ny, self.nz = nx, ny, nz
        self.gx, self.gy, self.gz = (lax.axis_index(a) for a in ("gx", "gy", "gz"))
        self.group = self.gx * ny + self.gy
        self.groups = nx * ny
        self.side = self.gz // (nz // 2)
        self.mid = nz // 2 - 1 + self.side
        self.far = self.side * (nz - 1)
        self.is_mid = self.gz == self.mid
        self.is_far = jnp.logical_and(self.gz == self.far, jnp.logical_not(self.is_mid))

    def member(self, offset):
        q = lax.rem(self.group + offset, self.groups)
        return q, q // self.ny, lax.rem(q, self.ny)


def block(start, size):
    return pl.ds(pl.multiple_of(start, size), size)


def remote(src, dst, send, recv, **device):
    return pltpu.make_async_remote_copy(
        src_ref=src, dst_ref=dst, send_sem=send, recv_sem=recv, device_id=device, device_id_type=MESH
    )


def column(row):
    n = row.shape[1]
    same = lax.broadcasted_iota(jnp.int32, (n, n), 0) == lax.broadcasted_iota(jnp.int32, (n, n), 1)
    return jnp.sum(jnp.where(same, row, 0.0), axis=1, keepdims=True)


def turn_in(slab, source, count):
    def body(i, carry):
        for u in range(8):
            channel = i * 8 + u
            for part in range(slab.shape[0]):
                slab.at[part][pl.ds(channel * PITCH, GROUP), :] = source(channel, part).astype(
                    jnp.float32
                )
        return carry

    lax.fori_loop(0, count // 8, body, 0)


def turn_out(slab, put, count):
    def body(i, carry):
        for u in range(8):
            channel = i * 8 + u
            for part in range(slab.shape[0]):
                rows = slab.at[part][pl.ds(channel * PITCH, GROUP), :]
                put(channel, part, rows.astype(jnp.bfloat16))
        return carry

    lax.fori_loop(0, count // 8, body, 0)


def get_rows(slab, row, count):
    return jnp.concatenate(
        [
            slab.at[part][pl.ds(row + u, count, stride=PITCH), :]
            for u in range(WIDE)
            for part in range(slab.shape[0])
        ],
        axis=1,
    )


def put_rows(slab, row, values):
    parts = slab.shape[0]
    for u in range(WIDE):
        for part in range(parts):
            lane = (u * parts + part) * LANES
            slab.at[part][pl.ds(row + u, values.shape[0], stride=PITCH), :] = values[
                :, lane : lane + LANES
            ]


def start(copies):
    for copy, _ in copies:
        copy.start()


def drain(copies):
    for copy, is_local in copies:
        if is_local:
            copy.wait()
        else:
            copy.wait_send()


def update_kernel(
    dims,
    pair_ref,
    mask_ref,
    gain_row_ref,
    mix_gain_ref,
    w0_ref,
    w1_ref,
    w2_ref,
    w3_ref,
    w4_ref,
    w5_ref,
    out_ref,
    raw_ref,
    left_ref,
    gate_ref,
    right,
    mix,
    ring,
    left,
    right_stage,
    left_stage,
    gate_stage,
    mix_stage,
    in_slab,
    out_slab,
    left_slab,
    weight,
    mix_weight,
    mix_gain_parts,
    mix_gain,
    raw_send,
    raw_recv,
    load_sem,
    small_send,
    small_recv,
    right_send,
    left_send,
    right_recv,
    left_recv,
    gate_sem,
    left_sem,
    mix_send,
    mix_recv,
    out_send,
    out_recv,
    credit,
):
    nx, ny, nz, near, away = dims
    at = Place(nx, ny, nz)
    c, rows, k = pair_ref.shape
    h_z, c_all = w0_ref.shape
    h = h_z * nz
    chunks = rows // GROUP
    half = chunks // 2
    own_rows = rows // 2
    steps = half
    per = near + away
    ahead = min(6, chunks)
    lag = min(LAG, steps)
    parts = k // LANES
    other = 1 - at.side

    def mid_of(side):
        return nz // 2 - 1 + side


    def chunk_of(t, side):
        return lax.rem(t + side * half, chunks)

    def raw_copy(t, side):
        chunk = chunk_of(t, side)
        where = block(chunk * GROUP, GROUP)
        return remote(
            pair_ref.at[:, where],
            raw_ref.at[block(at.gz * c, c), where],
            raw_send.at[t, side],
            raw_recv.at[chunk, at.gz],
            gz=mid_of(side),
        )

    def arrive(t):
        chunk = chunk_of(t, at.side)
        where = block(chunk * GROUP, GROUP)
        for o in range(1, nz):
            z = lax.rem(at.gz + o, nz)
            landed = raw_ref.at[block(z * c, c), where]
            remote(landed, landed, raw_send.at[t, 0], raw_recv.at[chunk, z], gz=z).wait_recv()

    def loads(t):
        slot = lax.rem(t, 2)
        where = block(chunk_of(t, at.side) * GROUP, GROUP)
        found = []
        for o in range(nz):
            z = lax.rem(at.gz + o, nz)
            src = pair_ref.at[:, where] if o == 0 else raw_ref.at[block(z * c, c), where]
            found.append(
                pltpu.make_async_copy(src, ring.at[slot, block(z * c, c)], load_sem.at[slot, o])
            )
        return found

    def small(z):
        sources = (w0_ref, w1_ref, w2_ref, w3_ref, w4_ref)
        found = [(src, weight.at[index, block(z * h_z, h_z)]) for index, src in enumerate(sources)]
        found.append((w5_ref, mix_weight.at[block(z * c, c)]))
        found.append((mix_gain_ref, mix_gain_parts.at[z]))
        return list(enumerate(found))

    def small_copies(side):
        return [
            (
                remote(
                    src, dst, small_send.at[side, i], small_recv.at[at.gz, i], gz=mid_of(side)
                ),
                False,
            )
            for i, (src, dst) in small(at.gz)
        ]

    def small_own():
        return [
            (pltpu.make_async_copy(src, dst, small_recv.at[at.gz, i]), True)
            for i, (src, dst) in small(at.gz)
        ]

    def small_arrive():
        drain(small_own())
        for o in range(1, nz):
            z = lax.rem(at.gz + o, nz)
            for i, (src, dst) in small(z):
                remote(src, dst, small_send.at[0, i], small_recv.at[z, i], gz=z).wait_recv()
        for z in range(nz):
            mix_gain[z * h_z : (z + 1) * h_z, :] = column(mix_gain_parts[z])


    def sends(stage, out, first, send, recv, slot):
        where = (block(first, GROUP), block(at.gx * k, k))
        found = []
        for o in range(at.groups):
            q, qx, qy = at.member(o)
            if o > 0:
                found.append(
                    (
                        remote(
                            stage.at[slot, pl.ds(q * per, near)],
                            out.at[(pl.ds(0, near),) + where],
                            send.at[slot, o],
                            recv.at[at.group],
                            gx=qx,
                            gy=qy,
                        ),
                        False,
                    )
                )
            if away:
                found.append(
                    (
                        remote(
                            stage.at[slot, pl.ds(q * per + near, away)],
                            out.at[(pl.ds(0, away),) + where],
                            send.at[slot, at.groups + o],
                            recv.at[at.group],
                            gx=qx,
                            gy=qy,
                            gz=at.far,
                        ),
                        False,
                    )
                )
        return found

    def right_first(t):
        return at.gy * rows + chunk_of(t, at.side) * GROUP

    def left_first(t):
        return at.gy * own_rows + t * GROUP

    def right_sends(t):
        slot = lax.rem(t, SLOTS)
        return sends(right_stage, right, right_first(t), right_send, right_recv, slot)

    def left_sends(t):
        slot = lax.rem(t, SLOTS)
        own = pltpu.make_async_copy(
            left_stage.at[slot, pl.ds(at.group * per, near)],
            left_ref.at[pl.ds(0, near), block(left_first(t), GROUP), block(at.gx * k, k)],
            left_send.at[slot, 0],
        )
        return sends(left_stage, left_ref, left_first(t), left_send, left_recv, slot) + [(own, True)]

    def gate_out(t):
        slot = lax.rem(t, 2)
        return pltpu.make_async_copy(
            gate_stage.at[slot], gate_ref.at[pl.ds(t * GROUP, GROUP)], gate_sem.at[slot]
        )

    def project(t, with_left):
        slot = lax.rem(t, SLOTS)
        gate_slot = lax.rem(t, 2)
        load_slot = lax.rem(t, 2)
        r0 = chunk_of(t, at.side) * GROUP
        gain = column(gain_row_ref[...])
        turn_in(
            in_slab,
            lambda channel, part: ring[load_slot, channel, :, part * LANES : (part + 1) * LANES],
            c_all,
        )

        def body(i, carry):
            r = i * WIDE
            normed = normalize(get_rows(in_slab, r, c_all), gain)
            mask = jnp.concatenate(
                [mask_ref[pl.ds(r0 + r + u, 1), :] for u in range(WIDE)], axis=1
            ).astype(jnp.float32)

            def part(index):
                return jnp.dot(weight[index], normed, preferred_element_type=jnp.float32)

            put_rows(out_slab, r, mask * jax.nn.sigmoid(part(3)) * part(2))
            if with_left:
                put_rows(left_slab, r, mask * jax.nn.sigmoid(part(1)) * part(0))
                gates = jax.nn.sigmoid(part(4)).astype(jnp.bfloat16)
                for u in range(WIDE):
                    gate_stage[gate_slot, r + u] = gates[:, u * k : (u + 1) * k]
            return carry

        lax.fori_loop(0, GROUP // WIDE, body, 0)

        def stage_into(stage):
            def put(head, part, values):
                stage[slot, head, :, part * LANES : (part + 1) * LANES] = values

            return put

        turn_out(out_slab, stage_into(right_stage), h)
        right[0:near, block(right_first(t), GROUP), block(at.gx * k, k)] = right_stage[
            slot, pl.ds(at.group * per, near)
        ]
        if with_left:
            turn_out(left_slab, stage_into(left_stage), h)

    def collect(heads, first_offset):
        for o in range(first_offset, at.groups):
            q, qx, qy = at.member(o)
            for out, size, recv in ((right, rows, right_recv), (left_ref, own_rows, left_recv)):
                whole = out.at[pl.ds(0, heads), block(qy * size, size), block(qx * k, k)]
                remote(whole, whole, gate_sem.at[0], recv.at[q], gz=at.mid).wait_recv()


    def left_loads(t, heads):
        slot = lax.rem(t, 2)
        return [
            pltpu.make_async_copy(
                left_ref.at[pl.ds(0, heads), block(y * own_rows + t * GROUP, GROUP)],
                left.at[slot, pl.ds(0, heads), pl.ds(y * GROUP, GROUP)],
                left_sem.at[slot, y],
            )
            for y in range(ny)
        ]

    def mix_sends(t, heads, shift, first_offset):
        slot = lax.rem(t, SLOTS)
        found = []
        for o in range(first_offset, at.groups):
            q, qx, qy = at.member(o)
            found.append(
                (
                    remote(
                        mix_stage.at[
                            slot, pl.ds(0, heads), block(qy * GROUP, GROUP), block(qx * k, k)
                        ],
                        mix.at[pl.ds(at.group * per + shift, heads), block(t * GROUP, GROUP)],
                        mix_send.at[slot, o],
                        mix_recv.at[t],
                        gx=qx,
                        gy=qy,
                        gz=at.mid,
                    ),
                    False,
                )
            )
        return found

    def multiply(t, heads, shift, first_offset, paced=False):
        slot = lax.rem(t, SLOTS)
        left_slot = lax.rem(t, 2)

        @pl.when(t + 1 < steps)
        def _():
            for copy in left_loads(t + 1, heads):
                copy.start()

        for copy in left_loads(t, heads):
            copy.wait()

        @pl.when(t >= SLOTS)
        def _():
            drain(mix_sends(t - SLOTS, heads, shift, first_offset))

        def body(head, carry):
            product = lax.dot_general(
                left[left_slot, head],
                right[head],
                (((1,), (1,)), ((), ())),
                preferred_element_type=jnp.float32,
            )
            mix_stage[slot, head] = product.astype(jnp.bfloat16)
            return carry

        lax.fori_loop(0, heads, body, 0)
        if paced:

            pl.semaphore_wait(credit, 1)

        start(mix_sends(t, heads, shift, first_offset))

    def multiply_end(heads, shift, first_offset):
        for t in range(max(steps - SLOTS, 0), steps):
            drain(mix_sends(t, heads, shift, first_offset))


    def gate_load(t):
        slot = lax.rem(t, 2)
        return pltpu.make_async_copy(
            gate_ref.at[pl.ds(t * GROUP, GROUP)], gate_stage.at[slot], gate_sem.at[slot]
        )

    def out_copies(t):
        slot = lax.rem(t, SLOTS)
        where = block(at.side * own_rows + t * GROUP, GROUP)
        own = pltpu.make_async_copy(
            right_stage.at[slot, block(at.gz * c, c)], out_ref.at[:, where], out_send.at[slot, 0]
        )
        found = [(own, True)]
        for o in range(1, nz):
            z = lax.rem(at.gz + o, nz)
            found.append(
                (
                    remote(
                        right_stage.at[slot, block(z * c, c)],
                        out_ref.at[:, where],
                        out_send.at[slot, o],
                        out_recv.at[at.side],
                        gz=z,
                    ),
                    False,
                )
            )
        return found

    def finish(t):
        slot = lax.rem(t, SLOTS)
        gate_slot = lax.rem(t, 2)
        here = block(t * GROUP, GROUP)
        if h > near:
            rest = mix.at[pl.ds(0, h - near), here]
            remote(rest, rest, out_send.at[0, 0], mix_recv.at[t], gz=at.mid).wait_recv()

        gain = mix_gain[...]
        turn_in(
            in_slab, lambda head, part: mix[head, here, part * LANES : (part + 1) * LANES], h
        )

        @pl.when(t + 1 < steps)
        def _():
            gate_load(t + 1).start()

        gate_load(t).wait()

        def body(i, carry):
            r = i * WIDE
            normed = normalize(get_rows(in_slab, r, h), gain)
            projected = jnp.dot(mix_weight[...], normed, preferred_element_type=jnp.float32)
            gates = jnp.concatenate([gate_stage[gate_slot, r + u] for u in range(WIDE)], axis=1)
            put_rows(out_slab, r, gates.astype(jnp.float32) * projected)
            return carry

        lax.fori_loop(0, GROUP // WIDE, body, 0)

        @pl.when(t >= SLOTS)
        def _():
            drain(out_copies(t - SLOTS))

        def put(channel, part, values):
            right_stage[slot, channel, :, part * LANES : (part + 1) * LANES] = values

        turn_out(out_slab, put, c_all)
        start(out_copies(t))


    @pl.when(jnp.logical_not(at.is_mid))
    def _():
        def begin(t, carry):
            raw_copy(t, 0).start()
            raw_copy(t, 1).start()
            return carry

        def end(t, carry):
            raw_copy(t, 0).wait_send()
            raw_copy(t, 1).wait_send()
            return carry

        for side in range(2):
            start(small_copies(side))
        lax.fori_loop(0, chunks, begin, 0)
        lax.fori_loop(0, chunks, end, 0)
        for side in range(2):
            drain(small_copies(side))

    if away:

        @pl.when(at.is_far)
        def _():
            collect(away, 0)
            for copy in left_loads(0, away):
                copy.start()

            def step(t, carry):
                multiply(t, away, near, 0, True)
                return carry

            lax.fori_loop(0, steps, step, 0)
            multiply_end(away, near, 0)

    @pl.when(at.is_mid)
    def _():
        start(small_own())
        start(small_copies(other))
        for t in range(ahead):
            raw_copy(t, other).start()
        small_arrive()
        arrive(0)
        for copy in loads(0):
            copy.start()

        def step(t, with_left):
            @pl.when(t + ahead < chunks)
            def _():
                raw_copy(t + ahead, other).start()

            @pl.when(t >= SLOTS)
            def _():
                drain(right_sends(t - SLOTS))
                if with_left:
                    drain(left_sends(t - SLOTS))

            if with_left:

                @pl.when(t >= 2)
                def _():
                    gate_out(t - 2).wait()

            for copy in loads(t):
                copy.wait()
            project(t, with_left)
            start(right_sends(t))
            if with_left:
                start(left_sends(t))
                gate_out(t).start()

            @pl.when(t + 1 < chunks)
            def _():
                arrive(t + 1)
                for copy in loads(t + 1):
                    copy.start()

        def first(t, carry):
            step(t, True)
            return carry

        def second(t, carry):
            step(t, False)
            return carry

        lax.fori_loop(0, half, first, 0)
        for t in range(max(half - 2, 0), half):
            gate_out(jnp.int32(t)).wait()
        gate_load(jnp.int32(0)).start()
        lax.fori_loop(half, chunks, second, 0)
        for t in range(max(half - SLOTS, 0), half):
            drain(left_sends(t))
        for t in range(max(chunks - SLOTS, 0), chunks):
            drain(right_sends(t))
        collect(near, 1)
        for copy in left_loads(0, near):
            copy.start()

        def both(t, carry):
            multiply(t, near, 0, 1)
            if away:

                pl.semaphore_signal(credit, inc=1, device_id={"gz": at.far}, device_id_type=MESH)

            slot = lax.rem(t, SLOTS)
            mix[pl.ds(at.group * per, near), block(t * GROUP, GROUP)] = mix_stage[
                slot, 0:near, block(at.gy * GROUP, GROUP), block(at.gx * k, k)
            ]

            @pl.when(t >= lag)
            def _():
                finish(t - lag)

            return carry

        def last(t, carry):
            finish(t)
            return carry

        lax.fori_loop(0, steps, both, 0)
        lax.fori_loop(steps - lag, steps, last, 0)
        multiply_end(near, 0, 1)
        for t in range(max(steps - SLOTS, 0), steps):
            drain(out_copies(t))
        drain(small_copies(other))

        def end(t, carry):
            raw_copy(t, other).wait_send()
            return carry

        lax.fori_loop(0, chunks, end, 0)

    for side in range(2):

        @pl.when(at.gz != mid_of(side))
        def _():
            where = out_ref.at[:, pl.ds(side * own_rows, own_rows)]
            remote(where, where, gate_sem.at[0], out_recv.at[side], gz=mid_of(side)).wait_recv()


def local(
    pair,
    pair_mask,
    in_gain,
    w_left,
    w_left_gate,
    w_right,
    w_right_gate,
    w_out_gate,
    out_gain,
    w_out,
):
    nx, ny, nz = (lax.axis_size(a) for a in ("gx", "gy", "gz"))
    c, rows, k = pair.shape
    c_all = c * nz
    h = w_left.shape[1] * nz
    groups = nx * ny
    per = h // groups
    away = 0 if nz < 4 else max(1, per * 5 // 16)
    near = per - away
    deep = max(near, away)
    dims = (nx, ny, nz, near, away)
    chunks = rows // GROUP
    steps = chunks // 2
    parts = k // LANES
    widest = max(h, c_all)

    anywhere = pl.BlockSpec(memory_space=pl.ANY)
    whole = pl.BlockSpec(memory_space=pltpu.VMEM)
    shape = lambda *dims: jax.ShapeDtypeStruct(dims, jnp.bfloat16)
    half = lambda *dims: pltpu.VMEM(dims, jnp.bfloat16)
    full = lambda *dims: pltpu.VMEM(dims, jnp.float32)
    sem = pltpu.SemaphoreType.DMA

    return pl.pallas_call(
        functools.partial(update_kernel, dims),
        out_shape=(
            shape(c, rows, k),
            shape(c_all, rows, k),
            shape(deep, ny * rows // 2, nx * k),
            shape(rows // 2, h, k),
        ),
        in_specs=[anywhere, whole, whole] + [anywhere] * 7,
        out_specs=(anywhere,) * 4,
        scratch_shapes=[
            half(deep, ny * rows, nx * k),
            half(h, rows // 2, k),
            half(2, c_all, GROUP, k),
            half(2, deep, ny * GROUP, nx * k),
            half(SLOTS, widest, GROUP, k),
            half(SLOTS, h, GROUP, k),
            half(2, GROUP, h, k),
            half(SLOTS, deep, ny * GROUP, ny * rows),
            full(parts, widest * PITCH, LANES),
            full(parts, widest * PITCH, LANES),
            full(parts, h * PITCH, LANES),
            half(5, h, c_all),
            half(c_all, h),
            full(nz, 1, h // nz),
            full(h, 1),
            sem((chunks, 2)),
            sem((chunks, nz)),
            sem((2, nz)),
            sem((2, 7)),
            sem((nz, 7)),
            sem((SLOTS, 2 * groups)),
            sem((SLOTS, 2 * groups)),
            sem((groups,)),
            sem((groups,)),
            sem((2,)),
            sem((2, ny)),
            sem((SLOTS, groups)),
            sem((steps,)),
            sem((SLOTS, nz)),
            sem((2,)),
            pltpu.SemaphoreType.REGULAR,
        ],
        compiler_params=pltpu.CompilerParams(has_side_effects=True, vmem_limit_bytes=VMEM_LIMIT),
    )(
        pair,
        pair_mask,
        in_gain[None, :],
        out_gain[None, :],
        w_left.T,
        w_left_gate.T,
        w_right.T,
        w_right_gate.T,
        w_out_gate.T,
        w_out.T,
    )[0]


def solution(mesh):
    placed = (
        P("gz", "gy", "gx"),
        P("gy", "gx"),
        P(),
        P(None, "gz"),
        P(None, "gz"),
        P(None, "gz"),
        P(None, "gz"),
        P(None, "gz"),
        P("gz"),
        P(None, "gz"),
    )
    return jax.shard_map(
        local, mesh=mesh, in_specs=placed, out_specs=P("gz", "gy", "gx"), check_vma=False
    )
```

```python
import functools

import jax
import jax.numpy as jnp
from jax import lax
from jax.experimental import pallas as pl
from jax.experimental.pallas import tpu as pltpu
from jax.sharding import PartitionSpec as P

epsilon = 1e-05
MESH = pl.DeviceIdType.MESH
LANES = 128
GROUP = 16
PITCH = GROUP + 1
SLOTS = 4
LAG = 2
WIDE = 2
VMEM_LIMIT = 67043328


def normalize(values, gain):
    average = jnp.mean(values, axis=0, keepdims=True)
    centered = values - average
    spread = jnp.mean(jnp.square(centered), axis=0, keepdims=True)
    return (centered * lax.rsqrt(spread + epsilon) * gain).astype(jnp.bfloat16)


class Place:
    def __init__(self, nx, ny, nz):
        self.nx, self.ny, self.nz = nx, ny, nz
        self.gx, self.gy, self.gz = (lax.axis_index(a) for a in ("gx", "gy", "gz"))
        self.group = self.gx * ny + self.gy
        self.groups = nx * ny
        self.side = self.gz // (nz // 2)
        self.mid = nz // 2 - 1 + self.side
        self.far = self.side * (nz - 1)
        self.is_mid = self.gz == self.mid
        self.is_far = jnp.logical_and(self.gz == self.far, jnp.logical_not(self.is_mid))

    def member(self, offset):
        q = lax.rem(self.group + offset, self.groups)
        return q, q // self.ny, lax.rem(q, self.ny)


def block(start, size):
    return pl.ds(pl.multiple_of(start, size), size)


def remote(src, dst, send, recv, **device):
    return pltpu.make_async_remote_copy(
        src_ref=src, dst_ref=dst, send_sem=send, recv_sem=recv, device_id=device, device_id_type=MESH
    )


def column(row):
    n = row.shape[1]
    same = lax.broadcasted_iota(jnp.int32, (n, n), 0) == lax.broadcasted_iota(jnp.int32, (n, n), 1)
    return jnp.sum(jnp.where(same, row, 0.0), axis=1, keepdims=True)


def turn_in(slab, source, count):
    def body(i, carry):
        for u in range(8):
            channel = i * 8 + u
            for part in range(slab.shape[0]):
                slab.at[part][pl.ds(channel * PITCH, GROUP), :] = source(channel, part).astype(
                    jnp.float32
                )
        return carry

    lax.fori_loop(0, count // 8, body, 0)


def turn_out(slab, put, count):
    def body(i, carry):
        for u in range(8):
            channel = i * 8 + u
            for part in range(slab.shape[0]):
                rows = slab.at[part][pl.ds(channel * PITCH, GROUP), :]
                put(channel, part, rows.astype(jnp.bfloat16))
        return carry

    lax.fori_loop(0, count // 8, body, 0)


def get_rows(slab, row, count):
    return jnp.concatenate(
        [
            slab.at[part][pl.ds(row + u, count, stride=PITCH), :]
            for u in range(WIDE)
            for part in range(slab.shape[0])
        ],
        axis=1,
    )


def put_rows(slab, row, values):
    parts = slab.shape[0]
    for u in range(WIDE):
        for part in range(parts):
            lane = (u * parts + part) * LANES
            slab.at[part][pl.ds(row + u, values.shape[0], stride=PITCH), :] = values[
                :, lane : lane + LANES
            ]


def start(copies):
    for copy, _ in copies:
        copy.start()


def drain(copies):
    for copy, is_local in copies:
        if is_local:
            copy.wait()
        else:
            copy.wait_send()


def update_kernel(
    dims,
    pair_ref,
    mask_ref,
    gain_row_ref,
    mix_gain_ref,
    w0_ref,
    w1_ref,
    w2_ref,
    w3_ref,
    w4_ref,
    w5_ref,
    out_ref,
    raw_ref,
    left_ref,
    gate_ref,
    right,
    mix,
    ring,
    left,
    right_stage,
    left_stage,
    gate_stage,
    mix_stage,
    in_slab,
    out_slab,
    left_slab,
    weight,
    mix_weight,
    mix_gain_parts,
    mix_gain,
    raw_send,
    raw_recv,
    load_sem,
    small_send,
    small_recv,
    right_send,
    left_send,
    right_recv,
    left_recv,
    gate_sem,
    left_sem,
    mix_send,
    mix_recv,
    out_send,
    out_recv,
    credit,
):
    nx, ny, nz, near, away = dims
    at = Place(nx, ny, nz)
    c, rows, k = pair_ref.shape
    h_z, c_all = w0_ref.shape
    h = h_z * nz
    chunks = rows // GROUP
    half = chunks // 2
    own_rows = rows // 2
    steps = half
    per = near + away
    ahead = min(6, chunks)
    lag = min(LAG, steps)
    parts = k // LANES
    other = 1 - at.side

    def mid_of(side):
        return nz // 2 - 1 + side


    def chunk_of(t, side):
        return lax.rem(t + side * half, chunks)

    def raw_copy(t, side):
        chunk = chunk_of(t, side)
        where = block(chunk * GROUP, GROUP)
        return remote(
            pair_ref.at[:, where],
            raw_ref.at[block(at.gz * c, c), where],
            raw_send.at[t, side],
            raw_recv.at[chunk, at.gz],
            gz=mid_of(side),
        )

    def arrive(t):
        chunk = chunk_of(t, at.side)
        where = block(chunk * GROUP, GROUP)
        for o in range(1, nz):
            z = lax.rem(at.gz + o, nz)
            landed = raw_ref.at[block(z * c, c), where]
            remote(landed, landed, raw_send.at[t, 0], raw_recv.at[chunk, z], gz=z).wait_recv()

    def loads(t):
        slot = lax.rem(t, 2)
        where = block(chunk_of(t, at.side) * GROUP, GROUP)
        found = []
        for o in range(nz):
            z = lax.rem(at.gz + o, nz)
            src = pair_ref.at[:, where] if o == 0 else raw_ref.at[block(z * c, c), where]
            found.append(
                pltpu.make_async_copy(src, ring.at[slot, block(z * c, c)], load_sem.at[slot, o])
            )
        return found

    def small(z):
        sources = (w0_ref, w1_ref, w2_ref, w3_ref, w4_ref)
        found = [(src, weight.at[index, block(z * h_z, h_z)]) for index, src in enumerate(sources)]
        found.append((w5_ref, mix_weight.at[block(z * c, c)]))
        found.append((mix_gain_ref, mix_gain_parts.at[z]))
        return list(enumerate(found))

    def small_copies(side):
        return [
            (
                remote(
                    src, dst, small_send.at[side, i], small_recv.at[at.gz, i], gz=mid_of(side)
                ),
                False,
            )
            for i, (src, dst) in small(at.gz)
        ]

    def small_own():
        return [
            (pltpu.make_async_copy(src, dst, small_recv.at[at.gz, i]), True)
            for i, (src, dst) in small(at.gz)
        ]

    def small_arrive():
        drain(small_own())
        for o in range(1, nz):
            z = lax.rem(at.gz + o, nz)
            for i, (src, dst) in small(z):
                remote(src, dst, small_send.at[0, i], small_recv.at[z, i], gz=z).wait_recv()
        for z in range(nz):
            mix_gain[z * h_z : (z + 1) * h_z, :] = column(mix_gain_parts[z])


    def sends(stage, out, first, send, recv, slot):
        where = (block(first, GROUP), block(at.gx * k, k))
        found = []
        for o in range(at.groups):
            q, qx, qy = at.member(o)
            if o > 0:
                found.append(
                    (
                        remote(
                            stage.at[slot, pl.ds(q * per, near)],
                            out.at[(pl.ds(0, near),) + where],
                            send.at[slot, o],
                            recv.at[at.group],
                            gx=qx,
                            gy=qy,
                        ),
                        False,
                    )
                )
            if away:
                found.append(
                    (
                        remote(
                            stage.at[slot, pl.ds(q * per + near, away)],
                            out.at[(pl.ds(0, away),) + where],
                            send.at[slot, at.groups + o],
                            recv.at[at.group],
                            gx=qx,
                            gy=qy,
                            gz=at.far,
                        ),
                        False,
                    )
                )
        return found

    def right_first(t):
        return at.gy * rows + chunk_of(t, at.side) * GROUP

    def left_first(t):
        return at.gy * own_rows + t * GROUP

    def right_sends(t):
        slot = lax.rem(t, SLOTS)
        return sends(right_stage, right, right_first(t), right_send, right_recv, slot)

    def left_sends(t):
        slot = lax.rem(t, SLOTS)
        own = pltpu.make_async_copy(
            left_stage.at[slot, pl.ds(at.group * per, near)],
            left_ref.at[pl.ds(0, near), block(left_first(t), GROUP), block(at.gx * k, k)],
            left_send.at[slot, 0],
        )
        return sends(left_stage, left_ref, left_first(t), left_send, left_recv, slot) + [(own, True)]

    def gate_out(t):
        slot = lax.rem(t, 2)
        return pltpu.make_async_copy(
            gate_stage.at[slot], gate_ref.at[pl.ds(t * GROUP, GROUP)], gate_sem.at[slot]
        )

    def project(t, with_left):
        slot = lax.rem(t, SLOTS)
        gate_slot = lax.rem(t, 2)
        load_slot = lax.rem(t, 2)
        r0 = chunk_of(t, at.side) * GROUP
        gain = column(gain_row_ref[...])
        turn_in(
            in_slab,
            lambda channel, part: ring[load_slot, channel, :, part * LANES : (part + 1) * LANES],
            c_all,
        )

        def body(i, carry):
            r = i * WIDE
            normed = normalize(get_rows(in_slab, r, c_all), gain)
            mask = jnp.concatenate(
                [mask_ref[pl.ds(r0 + r + u, 1), :] for u in range(WIDE)], axis=1
            ).astype(jnp.float32)

            def part(index):
                return jnp.dot(weight[index], normed, preferred_element_type=jnp.float32)

            put_rows(out_slab, r, mask * jax.nn.sigmoid(part(3)) * part(2))
            if with_left:
                put_rows(left_slab, r, mask * jax.nn.sigmoid(part(1)) * part(0))
                gates = jax.nn.sigmoid(part(4)).astype(jnp.bfloat16)
                for u in range(WIDE):
                    gate_stage[gate_slot, r + u] = gates[:, u * k : (u + 1) * k]
            return carry

        lax.fori_loop(0, GROUP // WIDE, body, 0)

        def stage_into(stage):
            def put(head, part, values):
                stage[slot, head, :, part * LANES : (part + 1) * LANES] = values

            return put

        turn_out(out_slab, stage_into(right_stage), h)
        right[0:near, block(right_first(t), GROUP), block(at.gx * k, k)] = right_stage[
            slot, pl.ds(at.group * per, near)
        ]
        if with_left:
            turn_out(left_slab, stage_into(left_stage), h)

    def collect(out, size, recv, heads, first_offset):
        for o in range(first_offset, at.groups):
            q, qx, qy = at.member(o)
            whole = out.at[pl.ds(0, heads), block(qy * size, size), block(qx * k, k)]
            remote(whole, whole, gate_sem.at[0], recv.at[q], gz=at.mid).wait_recv()

    def collect_left(heads, first_offset):
        collect(left_ref, own_rows, left_recv, heads, first_offset)
        for copy in left_loads(0, heads):
            copy.start()

    def collect_right(heads, first_offset):
        collect(right, rows, right_recv, heads, first_offset)


    def left_loads(t, heads):
        slot = lax.rem(t, 2)
        return [
            pltpu.make_async_copy(
                left_ref.at[pl.ds(0, heads), block(y * own_rows + t * GROUP, GROUP)],
                left.at[slot, pl.ds(0, heads), pl.ds(y * GROUP, GROUP)],
                left_sem.at[slot, y],
            )
            for y in range(ny)
        ]

    def mix_sends(t, heads, shift, first_offset):
        slot = lax.rem(t, SLOTS)
        found = []
        for o in range(first_offset, at.groups):
            q, qx, qy = at.member(o)
            found.append(
                (
                    remote(
                        mix_stage.at[
                            slot, pl.ds(0, heads), block(qy * GROUP, GROUP), block(qx * k, k)
                        ],
                        mix.at[pl.ds(at.group * per + shift, heads), block(t * GROUP, GROUP)],
                        mix_send.at[slot, o],
                        mix_recv.at[t],
                        gx=qx,
                        gy=qy,
                        gz=at.mid,
                    ),
                    False,
                )
            )
        return found

    def multiply(t, heads, shift, first_offset, paced=False):
        slot = lax.rem(t, SLOTS)
        left_slot = lax.rem(t, 2)

        @pl.when(t + 1 < steps)
        def _():
            for copy in left_loads(t + 1, heads):
                copy.start()

        for copy in left_loads(t, heads):
            copy.wait()

        @pl.when(t >= SLOTS)
        def _():
            drain(mix_sends(t - SLOTS, heads, shift, first_offset))

        def body(head, carry):
            product = lax.dot_general(
                left[left_slot, head],
                right[head],
                (((1,), (1,)), ((), ())),
                preferred_element_type=jnp.float32,
            )
            mix_stage[slot, head] = product.astype(jnp.bfloat16)
            return carry

        lax.fori_loop(0, heads, body, 0)
        if paced:

            pl.semaphore_wait(credit, 1)

        start(mix_sends(t, heads, shift, first_offset))

    def multiply_end(heads, shift, first_offset):
        for t in range(max(steps - SLOTS, 0), steps):
            drain(mix_sends(t, heads, shift, first_offset))


    def gate_load(t):
        slot = lax.rem(t, 2)
        return pltpu.make_async_copy(
            gate_ref.at[pl.ds(t * GROUP, GROUP)], gate_stage.at[slot], gate_sem.at[slot]
        )

    def out_copies(t):
        slot = lax.rem(t, SLOTS)
        where = block(at.side * own_rows + t * GROUP, GROUP)
        own = pltpu.make_async_copy(
            right_stage.at[slot, block(at.gz * c, c)], out_ref.at[:, where], out_send.at[slot, 0]
        )
        found = [(own, True)]
        for o in range(1, nz):
            z = lax.rem(at.gz + o, nz)
            found.append(
                (
                    remote(
                        right_stage.at[slot, block(z * c, c)],
                        out_ref.at[:, where],
                        out_send.at[slot, o],
                        out_recv.at[at.side],
                        gz=z,
                    ),
                    False,
                )
            )
        return found

    def finish(t):
        slot = lax.rem(t, SLOTS)
        gate_slot = lax.rem(t, 2)
        here = block(t * GROUP, GROUP)
        if h > near:
            rest = mix.at[pl.ds(0, h - near), here]
            remote(rest, rest, out_send.at[0, 0], mix_recv.at[t], gz=at.mid).wait_recv()

        gain = mix_gain[...]
        turn_in(
            in_slab, lambda head, part: mix[head, here, part * LANES : (part + 1) * LANES], h
        )

        @pl.when(t + 1 < steps)
        def _():
            gate_load(t + 1).start()

        gate_load(t).wait()

        def body(i, carry):
            r = i * WIDE
            normed = normalize(get_rows(in_slab, r, h), gain)
            projected = jnp.dot(mix_weight[...], normed, preferred_element_type=jnp.float32)
            gates = jnp.concatenate([gate_stage[gate_slot, r + u] for u in range(WIDE)], axis=1)
            put_rows(out_slab, r, gates.astype(jnp.float32) * projected)
            return carry

        lax.fori_loop(0, GROUP // WIDE, body, 0)

        @pl.when(t >= SLOTS)
        def _():
            drain(out_copies(t - SLOTS))

        def put(channel, part, values):
            right_stage[slot, channel, :, part * LANES : (part + 1) * LANES] = values

        turn_out(out_slab, put, c_all)
        start(out_copies(t))


    @pl.when(jnp.logical_not(at.is_mid))
    def _():
        def begin(t, carry):
            raw_copy(t, 0).start()
            raw_copy(t, 1).start()
            return carry

        def end(t, carry):
            raw_copy(t, 0).wait_send()
            raw_copy(t, 1).wait_send()
            return carry

        for side in range(2):
            start(small_copies(side))
        lax.fori_loop(0, chunks, begin, 0)
        lax.fori_loop(0, chunks, end, 0)
        for side in range(2):
            drain(small_copies(side))

    if away:

        @pl.when(at.is_far)
        def _():
            collect_left(away, 0)
            collect_right(away, 0)

            def step(t, carry):
                multiply(t, away, near, 0, True)
                return carry

            lax.fori_loop(0, steps, step, 0)
            multiply_end(away, near, 0)

    @pl.when(at.is_mid)
    def _():
        start(small_own())
        start(small_copies(other))
        for t in range(ahead):
            raw_copy(t, other).start()
        arrive(0)
        for copy in loads(0):
            copy.start()
        small_arrive()

        def step(t, with_left):
            @pl.when(t + ahead < chunks)
            def _():
                raw_copy(t + ahead, other).start()

            @pl.when(t >= SLOTS)
            def _():
                drain(right_sends(t - SLOTS))
                if with_left:
                    drain(left_sends(t - SLOTS))

            if with_left:

                @pl.when(t >= 2)
                def _():
                    gate_out(t - 2).wait()

            for copy in loads(t):
                copy.wait()
            project(t, with_left)
            start(right_sends(t))
            if with_left:
                start(left_sends(t))
                gate_out(t).start()

            @pl.when(t + 1 < chunks)
            def _():
                arrive(t + 1)
                for copy in loads(t + 1):
                    copy.start()

        def first(t, carry):
            step(t, True)
            return carry

        def second(t, carry):
            step(t, False)
            return carry

        lax.fori_loop(0, half, first, 0)
        for t in range(max(half - 2, 0), half):
            gate_out(jnp.int32(t)).wait()
        gate_load(jnp.int32(0)).start()
        lax.fori_loop(half, chunks, second, 0)
        for t in range(max(half - SLOTS, 0), half):
            drain(left_sends(t))
        collect_left(near, 1)
        for t in range(max(chunks - SLOTS, 0), chunks):
            drain(right_sends(t))
        collect_right(near, 1)

        def both(t, carry):
            multiply(t, near, 0, 1)
            if away:

                pl.semaphore_signal(credit, inc=1, device_id={"gz": at.far}, device_id_type=MESH)

            slot = lax.rem(t, SLOTS)
            mix[pl.ds(at.group * per, near), block(t * GROUP, GROUP)] = mix_stage[
                slot, 0:near, block(at.gy * GROUP, GROUP), block(at.gx * k, k)
            ]

            @pl.when(t >= lag)
            def _():
                finish(t - lag)

            return carry

        def last(t, carry):
            finish(t)
            return carry

        lax.fori_loop(0, steps, both, 0)
        lax.fori_loop(steps - lag, steps, last, 0)
        multiply_end(near, 0, 1)
        for t in range(max(steps - SLOTS, 0), steps):
            drain(out_copies(t))
        drain(small_copies(other))

        def end(t, carry):
            raw_copy(t, other).wait_send()
            return carry

        lax.fori_loop(0, chunks, end, 0)

    for side in range(2):

        @pl.when(at.gz != mid_of(side))
        def _():
            where = out_ref.at[:, pl.ds(side * own_rows, own_rows)]
            remote(where, where, gate_sem.at[0], out_recv.at[side], gz=mid_of(side)).wait_recv()


def local(
    pair,
    pair_mask,
    in_gain,
    w_left,
    w_left_gate,
    w_right,
    w_right_gate,
    w_out_gate,
    out_gain,
    w_out,
):
    nx, ny, nz = (lax.axis_size(a) for a in ("gx", "gy", "gz"))
    c, rows, k = pair.shape
    c_all = c * nz
    h = w_left.shape[1] * nz
    groups = nx * ny
    per = h // groups
    away = 0 if nz < 4 else max(1, per * 5 // 16)
    near = per - away
    deep = max(near, away)
    dims = (nx, ny, nz, near, away)
    chunks = rows // GROUP
    steps = chunks // 2
    parts = k // LANES
    widest = max(h, c_all)

    anywhere = pl.BlockSpec(memory_space=pl.ANY)
    whole = pl.BlockSpec(memory_space=pltpu.VMEM)
    shape = lambda *dims: jax.ShapeDtypeStruct(dims, jnp.bfloat16)
    half = lambda *dims: pltpu.VMEM(dims, jnp.bfloat16)
    full = lambda *dims: pltpu.VMEM(dims, jnp.float32)
    sem = pltpu.SemaphoreType.DMA

    return pl.pallas_call(
        functools.partial(update_kernel, dims),
        out_shape=(
            shape(c, rows, k),
            shape(c_all, rows, k),
            shape(deep, ny * rows // 2, nx * k),
            shape(rows // 2, h, k),
        ),
        in_specs=[anywhere, whole, whole] + [anywhere] * 7,
        out_specs=(anywhere,) * 4,
        scratch_shapes=[
            half(deep, ny * rows, nx * k),
            half(h, rows // 2, k),
            half(2, c_all, GROUP, k),
            half(2, deep, ny * GROUP, nx * k),
            half(SLOTS, widest, GROUP, k),
            half(SLOTS, h, GROUP, k),
            half(2, GROUP, h, k),
            half(SLOTS, deep, ny * GROUP, ny * rows),
            full(parts, widest * PITCH, LANES),
            full(parts, widest * PITCH, LANES),
            full(parts, h * PITCH, LANES),
            half(5, h, c_all),
            half(c_all, h),
            full(nz, 1, h // nz),
            full(h, 1),
            sem((chunks, 2)),
            sem((chunks, nz)),
            sem((2, nz)),
            sem((2, 7)),
            sem((nz, 7)),
            sem((SLOTS, 2 * groups)),
            sem((SLOTS, 2 * groups)),
            sem((groups,)),
            sem((groups,)),
            sem((2,)),
            sem((2, ny)),
            sem((SLOTS, groups)),
            sem((steps,)),
            sem((SLOTS, nz)),
            sem((2,)),
            pltpu.SemaphoreType.REGULAR,
        ],
        compiler_params=pltpu.CompilerParams(has_side_effects=True, vmem_limit_bytes=VMEM_LIMIT),
    )(
        pair,
        pair_mask,
        in_gain[None, :],
        out_gain[None, :],
        w_left.T,
        w_left_gate.T,
        w_right.T,
        w_right_gate.T,
        w_out_gate.T,
        w_out.T,
    )[0]


def solution(mesh):
    placed = (
        P("gz", "gy", "gx"),
        P("gy", "gx"),
        P(),
        P(None, "gz"),
        P(None, "gz"),
        P(None, "gz"),
        P(None, "gz"),
        P(None, "gz"),
        P("gz"),
        P(None, "gz"),
    )
    return jax.shard_map(
        local, mesh=mesh, in_specs=placed, out_specs=P("gz", "gy", "gx"), check_vma=False
    )
```
